32 devices in a mesh: section: 4 (over y, core), tensor: 8 (over z, x).
Axes of the slice: x: 2, y: 2, z: 4, core: 2. Of those that a mesh axis runs over, the one named last changes fastest.
Arguments:
- saved_inputs: bfloat16 [4, 4, 256, 1024], P('section', None, 'tensor'), may hold values from -6 to 6
- slot_index: int32 [4, 3], P('section'), may hold values from 0 to 3
- example_lengths: int32 [4, 3, 2], P('section'), may hold values from 1 to 192, 256 in all within a row
- first_grads: bfloat16 [4, 256, 1024], P('section', 'tensor'), may hold values from -6 to 6
- loss_grads: bfloat16 [2, 256, 1024], P(None, 'tensor'), may hold values from -6 to 6
- w_in: bfloat16 [4, 1024, 32768], P('section', None, 'tensor'), may hold values from -0.1875 to 0.1875
- w_out: bfloat16 [4, 32768, 1024], P('section', 'tensor'), may hold values from -0.03125 to 0.03125
Outputs:
- grad_in: bfloat16 [4, 1024, 32768], P('section', None, 'tensor')
- grad_out: bfloat16 [4, 32768, 1024], P('section', 'tensor')
- input_grads: bfloat16 [4, 3, 256, 1024], P('section', None, 'tensor')
The draws below stay inside these ranges and needn't reach their ends.
Inputs may be any that keep to these rules, and one draw needn't show every extreme that they name: `example_lengths`: the 2 lengths of one microbatch sum to 256.
All inputs are finite; a program needn't handle non-finite values.
Results may differ from the reference program's by a relative error of at most 0.0095.
Values may be sent and summed in bfloat16 or wider, within the bound.
A program may use at most 128 MiB of HBM per device.

```python
import math
import jax
import jax.numpy as jnp
import numpy as np
from jax import lax

D = 1024
FF = 32768
TOK_MB = 256
EXAMPLES = 2
SLOTS = 3
BUF = 4
MOST = 192
SECTIONS = 4


def plant(drawn, stream_key, low, high):
    shape = drawn.shape
    place = [jax.random.randint(jax.random.fold_in(stream_key, axis), (), 0, shape[axis]) for axis in range(len(shape))]
    drawn = drawn.at[tuple(place)].set(low)
    longest = shape.index(max(shape))
    place[longest] = (place[longest] + 1) % shape[longest]
    return drawn.at[tuple(place)].set(high)


def steps_of(own_key, dims, shards, smallest, high):
    def one(axis_at, shards_of):
        draws = jax.random.uniform(jax.random.fold_in(jax.random.fold_in(own_key, 6), axis_at), (shards_of,), jnp.float32, smallest / len(shards), high / len(shards))
        return jnp.repeat(jnp.exp(draws), dims[axis_at] // shards_of).reshape((-1,) + (1,) * (len(dims) - axis_at - 1))

    loudness = one(*shards[0])
    for cut in shards[1:]:
        loudness = loudness * one(*cut)
    return loudness


def split_up(count, total, most, lean):
    loads = [(1 << 20) // math.isqrt(grade ** lean) + 1 for grade in range(2, count + 1)]
    surplus, holding = total - most - (count - 1), [1] * (count - 1)
    while surplus > 0:
        free = [i for i in range(count - 1) if holding[i] < most]
        pool, left = sum([loads[i] for i in free]), surplus
        for i in free:
            addition = min(most - holding[i], max(1, left * loads[i] // pool), surplus)
            holding[i] = holding[i] + addition
            surplus = surplus - addition
    return np.array([most] + holding)


def uneven(rng, count, total, most, skew):
    if count == 2:
        one = jax.random.randint(rng, (), max(1, total - most), min(most, total - 1) + 1)
        return jnp.stack([one, total - one])
    sizes = jnp.asarray(split_up(count, total, most, skew), jnp.int32)
    pairs = (count - 1) // 2
    giver, sink = sizes[1:1 + 2 * pairs:2], sizes[2:2 + 2 * pairs:2]
    slack = jnp.minimum(giver - 1, most - sink)
    passed = jax.random.randint(jax.random.fold_in(rng, 1), (pairs,), 0, 1 << 20) % (slack + 1)
    sizes = sizes.at[1:1 + 2 * pairs:2].set(giver - passed).at[2:2 + 2 * pairs:2].set(sink + passed)
    return sizes[jax.random.permutation(jax.random.fold_in(rng, 2), count)]


def noise(rng, shape, spread, limit, split=(), kind=jnp.bfloat16):
    entries = spread * jax.random.normal(rng, shape, jnp.float32)
    if split:
        entries = entries * steps_of(rng, shape, split, -0.22, 0.18)
    return jnp.clip(entries, -limit, limit).astype(kind)


def setup_inputs(seed: int = 0) -> dict:
    key_of = jax.random.split(jax.random.key(seed), 8)
    saved_inputs = noise(key_of[0], (SECTIONS, BUF, TOK_MB, D), 1.0, 6.0, ((0, 4), (2, 8)))
    slot_index = plant(jax.random.randint(key_of[1], (SECTIONS, SLOTS), 0, BUF), jax.random.fold_in(key_of[1], 1), 0, BUF - 1).astype(jnp.int32)
    example_lengths = jax.vmap(lambda own: uneven(own, EXAMPLES, TOK_MB, MOST, 2))(jax.random.split(key_of[2], SECTIONS * SLOTS)).reshape((SECTIONS, SLOTS, EXAMPLES)).astype(jnp.int32)
    first_grads = noise(key_of[3], (SECTIONS, TOK_MB, D), 1.0, 6.0, ((0, 4), (1, 8)))
    loss_grads = noise(key_of[4], (SLOTS - 1, TOK_MB, D), 1.0, 6.0, ((1, 8),))
    w_in = noise(key_of[5], (SECTIONS, D, FF), D ** -0.5, 0.1875, ((0, 4), (2, 8)))
    w_out = noise(key_of[6], (SECTIONS, FF, D), FF ** -0.5, 0.03125, ((0, 4), (1, 8)))
    return dict(saved_inputs=saved_inputs, slot_index=slot_index, example_lengths=example_lengths, first_grads=first_grads, loss_grads=loss_grads, w_in=w_in, w_out=w_out)


GAMMA = 0.01

def membership(lengths, tokens):
    ends = jnp.cumsum(lengths)
    position = jnp.arange(tokens, dtype=jnp.int32)
    example_id = lax.optimization_barrier(jnp.sum((position[:, None] >= ends[None, :-1]).astype(jnp.int32), axis=1))
    labels = jnp.arange(lengths.shape[0], dtype=jnp.int32)
    return (example_id[:, None] == labels[None, :]).astype(jnp.float32)

def section_step(inputs, grads, first, second, lengths):
    z = jnp.dot(inputs, first, preferred_element_type=jnp.float32)
    relu = jnp.maximum(z, 0.0)
    hidden = (relu * relu).astype(jnp.bfloat16)
    back = jnp.dot(grads, second.T, preferred_element_type=jnp.float32)
    dz = (2.0 * relu * back).astype(jnp.bfloat16)
    dx = (grads.astype(jnp.float32) + jnp.dot(dz, first.T, preferred_element_type=jnp.float32)).astype(jnp.bfloat16)
    member = membership(lengths, inputs.shape[0])
    gram_x = jnp.dot(inputs, inputs.T, preferred_element_type=jnp.float32)
    gram_z = jnp.dot(dz, dz.T, preferred_element_type=jnp.float32)
    gram_h = jnp.dot(hidden, hidden.T, preferred_element_type=jnp.float32)
    gram_y = jnp.dot(grads, grads.T, preferred_element_type=jnp.float32)
    paired = gram_x * gram_z + gram_h * gram_y
    squares = lax.optimization_barrier(jnp.sum(member * jnp.dot(paired, member, precision=lax.Precision.HIGHEST), axis=0))
    factor = 1.0 / (jnp.sqrt(squares / (D * FF)) + GAMMA)
    token_factor = lax.optimization_barrier(jnp.sum(member * factor[None, :], axis=1))
    dzc = (dz.astype(jnp.float32) * token_factor[:, None]).astype(jnp.bfloat16)
    dyc = (grads.astype(jnp.float32) * token_factor[:, None]).astype(jnp.bfloat16)
    g_first = jnp.dot(inputs.T, dzc, preferred_element_type=jnp.float32)
    g_second = jnp.dot(hidden.T, dyc, preferred_element_type=jnp.float32)
    return (dx, g_first, g_second)

def reference(saved_inputs, slot_index, example_lengths, first_grads, loss_grads, w_in, w_out):
    section_count = w_in.shape[0]
    slot_count = slot_index.shape[1]
    acc_first = [jnp.zeros((D, FF), jnp.float32) for s in range(section_count)]
    acc_second = [jnp.zeros((FF, D), jnp.float32) for s in range(section_count)]
    previous = [None] * section_count
    results = [[None] * slot_count for s in range(section_count)]
    for slot in range(slot_count):
        current = [None] * section_count
        for section in range(section_count):
            if slot == 0:
                grads = first_grads[section]
            elif section == section_count - 1:
                grads = loss_grads[slot - 1]
            else:
                grads = previous[section + 1]
            inputs = lax.dynamic_index_in_dim(saved_inputs[section], slot_index[section, slot].astype(jnp.int32), 0, keepdims=False)
            dx, g_first, g_second = section_step(inputs, grads, w_in[section], w_out[section], example_lengths[section, slot])
            acc_first[section] = acc_first[section] + g_first
            acc_second[section] = acc_second[section] + g_second
            current[section] = dx
            results[section][slot] = dx
        previous = current
    grad_in = jnp.stack(acc_first).astype(jnp.bfloat16)
    grad_out = jnp.stack(acc_second).astype(jnp.bfloat16)
    input_grads = jnp.stack([jnp.stack(row) for row in results])
    return (grad_in, grad_out, input_grads)
```

```python
import functools

import jax
import jax.numpy as jnp
from jax import lax
from jax.experimental import pallas as pl
from jax.experimental.pallas import tpu as pltpu
from jax.sharding import PartitionSpec as P

GAMMA = 0.01
F32 = jnp.float32
BF16 = jnp.bfloat16
MESH = pl.DeviceIdType.MESH
NT = (((1,), (1,)), ((), ()))
TN = (((0,), (0,)), ((), ()))


def dot(a, b, dims):
    return lax.dot_general(a, b, dims, preferred_element_type=F32)


def chain_kernel(
    cfg,
    index_ref, lengths_ref, saved_ref, first_ref, loss_ref, win_hbm, wout_hbm,
    xct_hbm, dyc_hbm, h_hbm, dz_hbm, res_hbm,
    win, wout, xg, dyb, h, dz, rbuf, acc, own, rxs, rxr, rzs, rzr, res, sqs, sqr, xct, dyc,
    w_sem, ag_send, ag_recv, fw_send, fw_recv, rx_send, rx_recv, rz_send, rz_recv,
    sh_send, sh_recv, af_send, af_recv, sq_send, sq_recv, out_sem,
):
    sections, parts, nz, slots, rows, width, local, chunks, examples, hidden_all = cfg
    cols = width // chunks
    tokens = parts * rows
    tile = min(512, local)
    tiles = local // tile
    s = lax.axis_index("section")
    p = lax.axis_index("tensor")
    z = p // 2
    x = p % 2
    is_last = s == sections - 1
    partner = {"section": s, "tensor": z * 2 + (1 - x)}

    def zpeer(j):
        return {"section": s, "tensor": ((z + j) % nz) * 2 + x}

    def behind(j):
        return {"section": s - 1, "tensor": ((z + j) % nz) * 2 + x}

    pieces = 4
    span_in, span_out = local // pieces, local // pieces
    for k in range(pieces):
        pltpu.make_async_copy(win_hbm.at[0, :, pl.ds(k * span_in, span_in)], win.at[:, pl.ds(k * span_in, span_in)], w_sem.at[0, k]).start()
    for k in range(pieces):
        pltpu.make_async_copy(wout_hbm.at[0, pl.ds(k * span_out, span_out)], wout.at[pl.ds(k * span_out, span_out)], w_sem.at[1, k]).start()

    for t in range(slots):
        xg[t, z, x] = saved_ref[0, index_ref[0, t]]
    for c in range(chunks):
        dyb[0, c, z, x] = first_ref[0, :, pl.ds(c * cols, cols)]

    @pl.when(is_last)
    def _():
        for t in range(1, slots):
            for c in range(chunks):
                dyb[t, c, z, x] = loss_ref[t - 1, :, pl.ds(c * cols, cols)]

    barrier = pltpu.get_barrier_semaphore()
    for j in range(1, parts):
        pl.semaphore_signal(barrier, inc=1, device_id={"section": s, "tensor": (p + j) % parts}, device_id_type=MESH)

    for side in (1, sections - 1):
        for j in range(nz):
            pl.semaphore_signal(barrier, inc=1, device_id={"section": (s + side) % sections, "tensor": ((z + j) % nz) * 2 + x}, device_id_type=MESH)
    pl.semaphore_wait(barrier, parts - 1 + 2 * nz)

    def block(k, source):
        if k < slots:
            return xg.at[k, source, x]
        return dyb.at[k - slots, :, source, x]

    def ag_copy(k, j, to_partner):
        if to_partner:
            ref = block(k, (z + nz - j) % nz)
            return pltpu.make_async_remote_copy(ref, ref, fw_send.at[k, j], fw_recv.at[k, j], device_id=partner, device_id_type=MESH)
        ref = block(k, z)
        return pltpu.make_async_remote_copy(ref, ref, ag_send.at[k, j], ag_recv.at[k, j], device_id=zpeer(j), device_id_type=MESH)

    def ag_open(k):
        for j in range(1, nz):
            ag_copy(k, j, False).start()

    def ag_forward(k):
        ag_copy(k, 0, True).start()
        for j in range(1, nz):
            ag_copy(k, j, False).wait_recv()
            ag_copy(k, j, True).start()

    def ag_finish(k):
        for j in range(nz):
            ag_copy(k, j, True).wait_recv()

    def ag_drain(k):
        for j in range(nz):
            if j:
                ag_copy(k, j, False).wait_send()
            ag_copy(k, j, True).wait_send()

    def z_tiles(t, lo, hi):
        def body(i, carry):
            at = pl.ds(pl.multiple_of(i * tile, tile), tile)
            zz = jnp.dot(xg[t].reshape(tokens, width), win[:, at], preferred_element_type=F32)
            r = jnp.maximum(zz, 0.0)
            rbuf[:, at] = r
            h[t, :, at] = (r * r).astype(BF16)
            return carry

        lax.fori_loop(lo, hi, body, 0)

    def back_all(t):
        def body(i, carry):
            at = pl.ds(pl.multiple_of(i * tile, tile), tile)
            grads = jnp.concatenate([dyb[t, c].reshape(tokens, cols) for c in range(chunks)], axis=1)
            dh = dot(grads, wout[at, :], NT)
            dz[t, :, at] = (2.0 * rbuf[:, at] * dh).astype(BF16)
            return carry

        lax.fori_loop(0, tiles, body, 0)

    def back_chunk(t, c, mode):
        def body(i, carry):
            at = pl.ds(pl.multiple_of(i * tile, tile), tile)
            dh = dot(dyb[t, c].reshape(tokens, cols), wout[at, c * cols:(c + 1) * cols], NT)
            if mode > 0:
                dh = dh + acc[:, at]
            if mode < 2:
                acc[:, at] = dh
            else:
                dz[t, :, at] = (2.0 * rbuf[:, at] * dh).astype(BF16)
            return carry

        lax.fori_loop(0, tiles, body, 0)

    def rx_copy(t, c):
        return pltpu.make_async_remote_copy(rxs.at[t, c], rxr.at[t, c], rx_send.at[t, c], rx_recv.at[t, c], device_id=partner, device_id_type=MESH)

    def rz_copy(t, c, j):
        return pltpu.make_async_remote_copy(rzs.at[t, c, (z + j) % nz], rzr.at[t, c, j], rz_send.at[t, c, j], rz_recv.at[t, c, j], device_id=zpeer(j), device_id_type=MESH)

    def sh_copy(t, c, j):
        return pltpu.make_async_remote_copy(res.at[t, c], dyb.at[t + 1, c, z, x], sh_send.at[t, c, j], sh_recv.at[t, c, j], device_id=behind(j), device_id_type=MESH)

    def af_copy(t, c):
        ref = dyb.at[t + 1, c, :, x]
        return pltpu.make_async_remote_copy(ref, ref, af_send.at[t, c], af_recv.at[t, c], device_id=partner, device_id_type=MESH)

    def over_chunks(body):
        def step(c, carry):
            body(c)
            return carry

        lax.fori_loop(0, chunks, step, 0)

    def partial_dx(t):
        def body(c):
            wide = win[pl.ds(pl.multiple_of(c * cols, cols), cols), :]
            part = dot(dz[t], wide, NT).reshape(nz, 2, rows, cols)
            first_half, second_half = part[:, 0], part[:, 1]
            mine = jnp.where(x == 0, first_half, second_half)
            other = jnp.where(x == 0, second_half, first_half)
            own[c] = mine
            rxs[t, c] = other.astype(BF16)
            rx_copy(t, c).start()

        over_chunks(body)

    def pair_sum(t, c):
        rx_copy(t, c).wait_recv()
        total = own[c] + rxr[t, c].astype(F32)
        own[c] = total
        rzs[t, c] = total.astype(BF16)
        for j in range(1, nz):
            rz_copy(t, c, j).start()

    def line_sum(t, c):
        total = own[c, z] + dyb[t, c, z, x].astype(F32)
        for j in range(1, nz):
            rz_copy(t, c, j).wait_recv()
            total = total + rzr[t, c, j].astype(F32)
        res[t, c] = total.astype(BF16)
        if t + 1 < slots:
            @pl.when(s > 0)
            def _():
                for j in range(nz):
                    sh_copy(t, c, j).start()

    def hand_over(t, c):
        for j in range(nz):
            sh_copy(t, c, j).wait_recv()
        af_copy(t, c).start()

    def example_mask(t):
        position = lax.broadcasted_iota(jnp.int32, (tokens, 1), 0)
        across = lax.broadcasted_iota(jnp.int32, (1, tokens), 1)
        down, along = [], []
        start = jnp.int32(0)
        for e in range(examples):
            stop = start + lengths_ref[0, t, e]
            if e == examples - 1:
                stop = jnp.int32(tokens)
            down.append((position >= start) & (position < stop))
            along.append((across >= start) & (across < stop))
            start = stop
        return down, along

    def sq_copy(t, j):
        return pltpu.make_async_remote_copy(sqs.at[t], sqr.at[t, j], sq_send.at[t, j], sq_recv.at[t, j], device_id={"section": s, "tensor": (p + j) % parts}, device_id_type=MESH)

    def squares(t):
        inputs = xg[t].reshape(tokens, width)
        grads = jnp.concatenate([dyb[t, c].reshape(tokens, cols) for c in range(chunks)], axis=1)
        paired = dot(inputs, inputs, NT) * dot(dz[t], dz[t], NT) + dot(h[t], h[t], NT) * dot(grads, grads, NT)
        down, along = example_mask(t)
        row = lax.broadcasted_iota(jnp.int32, (8, 128), 0)
        out = jnp.zeros((8, 128), F32)
        for e in range(examples):
            kept = jnp.where(down[e], paired, 0.0)
            kept = jnp.where(along[e], kept, 0.0)
            value = jnp.sum(jnp.sum(kept, axis=0, keepdims=True), axis=1, keepdims=True)
            out = jnp.where(row == e, value, out)
        sqs[t] = out
        for j in range(1, parts):
            sq_copy(t, j).start()

    def out_copy(t, k):
        source, target = ((h, h_hbm), (dz, dz_hbm), (dyc, dyc_hbm), (xct, xct_hbm))[k]
        return pltpu.make_async_copy(source.at[t], target.at[t], out_sem.at[t, k])

    def scale(t):
        total = sqs[t]
        for j in range(1, parts):
            sq_copy(t, j).wait_recv()
            total = total + sqr[t, j]
        factor = 1.0 / (jnp.sqrt(total / (width * hidden_all)) + GAMMA)
        down, _ = example_mask(t)
        per_token = jnp.zeros((tokens, 1), F32)
        for e in range(examples):
            per_token = jnp.where(down[e], factor[e:e + 1, 0:1], per_token)
        scaled = xg[t].reshape(tokens, width).astype(F32) * per_token
        xct[t] = scaled.T.astype(BF16)
        for c in range(chunks):
            dyc[t, :, pl.ds(c * cols, cols)] = (dyb[t, c].reshape(tokens, cols).astype(F32) * per_token).astype(BF16)
        out_copy(t, 2).start()
        out_copy(t, 3).start()

    ag_open(0)
    ag_open(slots)
    ag_open(1)

    @pl.when(is_last)
    def _():
        ag_open(slots + 1)

    for t in range(2, slots):
        ag_open(t)

    @pl.when(is_last)
    def _():
        for t in range(2, slots):
            ag_open(slots + t)

    ag_forward(0)
    ag_forward(slots)
    for k in range(pieces):
        pltpu.make_async_copy(win_hbm.at[0, :, pl.ds(k * span_in, span_in)], win.at[:, pl.ds(k * span_in, span_in)], w_sem.at[0, k]).wait()
    for k in range(pieces):
        pltpu.make_async_copy(wout_hbm.at[0, pl.ds(k * span_out, span_out)], wout.at[pl.ds(k * span_out, span_out)], w_sem.at[1, k]).wait()
    ag_finish(0)
    z_tiles(0, 0, tiles)
    ag_finish(slots)
    back_all(0)

    for t in range(slots):
        more = t + 1 < slots
        partial_dx(t)
        out_copy(t, 0).start()
        out_copy(t, 1).start()
        squares(t)
        if more:
            ag_forward(t + 1)

            @pl.when(is_last)
            def _():
                ag_forward(slots + t + 1)

        over_chunks(lambda c: pair_sum(t, c))
        if more:
            ag_finish(t + 1)
            z_tiles(t + 1, 0, tiles)
        scale(t)
        over_chunks(lambda c: line_sum(t, c))
        if more:
            @pl.when(s < sections - 1)
            def _():
                over_chunks(lambda c: hand_over(t, c))

            @pl.when(is_last)
            def _():
                ag_finish(slots + t + 1)

            for c in range(chunks):
                @pl.when(s < sections - 1)
                def _():
                    af_copy(t, c).wait_recv()

                back_chunk(t + 1, c, 0 if c == 0 else (2 if c == chunks - 1 else 1))

    copies = []
    for t in range(slots):
        for c in range(chunks):
            copy = pltpu.make_async_copy(res.at[t, c], res_hbm.at[t, :, pl.ds(c * cols, cols)], out_sem.at[t, 4 + c])
            copy.start()
            copies.append(copy)
    for t in range(slots):
        ag_drain(t)
    ag_drain(slots)

    @pl.when(is_last)
    def _():
        for t in range(1, slots):
            ag_drain(slots + t)

    for t in range(slots):
        def drain(c):
            rx_copy(t, c).wait_send()
            for j in range(1, nz):
                rz_copy(t, c, j).wait_send()

        over_chunks(drain)
        for j in range(1, parts):
            sq_copy(t, j).wait_send()
        if t + 1 < slots:
            @pl.when(s > 0)
            def _():
                def drain_shift(c):
                    for j in range(nz):
                        sh_copy(t, c, j).wait_send()

                over_chunks(drain_shift)

            @pl.when(s < sections - 1)
            def _():
                over_chunks(lambda c: af_copy(t, c).wait_send())
    for t in range(slots):
        for k in range(4):
            out_copy(t, k).wait()
    for copy in copies:
        copy.wait()


def grads_kernel(xct_ref, dyc_ref, h_ref, dz_ref, res_ref, gin_ref, gout_ref, out_ref):
    slots = xct_ref.shape[0]
    lhs = jnp.concatenate([xct_ref[t] for t in range(slots)], axis=1)
    tokens, block = h_ref.shape[1:]
    dzs = dz_ref[...].reshape(slots * tokens, block)
    gin_ref[0] = jnp.dot(lhs, dzs, preferred_element_type=F32).astype(BF16)
    hs = h_ref[...].reshape(slots * tokens, block)
    dycs = dyc_ref[...].reshape(slots * tokens, dyc_ref.shape[2])
    gout_ref[0] = dot(hs, dycs, TN).astype(BF16)

    @pl.when(pl.program_id(0) == 0)
    def _():
        out_ref[0] = res_ref[...]


def fast_device(sections, saved_inputs, slot_index, example_lengths, first_grads, loss_grads, w_in, w_out):
    parts = lax.axis_size("tensor")
    slots = loss_grads.shape[0] + 1
    rows, width = first_grads.shape[1:]
    local = w_in.shape[2]
    nz = parts // 2
    tokens = parts * rows
    examples = example_lengths.shape[2]
    chunks = max(1, width // 256)
    cols = width // chunks
    cfg = (sections, parts, nz, slots, rows, width, local, chunks, examples, local * parts)
    hbm = pl.BlockSpec(memory_space=pl.ANY)
    vmem = pl.BlockSpec(memory_space=pltpu.VMEM)
    smem = pl.BlockSpec(memory_space=pltpu.SMEM)
    dma = pltpu.SemaphoreType.DMA
    sds = jax.ShapeDtypeStruct
    flops = 2 * tokens * width * local * slots * 3
    xct, dyc, h, dz, res = pl.pallas_call(
        functools.partial(chain_kernel, cfg),
        out_shape=(
            sds((slots, width, tokens), BF16),
            sds((slots, tokens, width), BF16),
            sds((slots, tokens, local), BF16),
            sds((slots, tokens, local), BF16),
            sds((slots, rows, width), BF16),
        ),
        in_specs=[smem, smem, vmem, vmem, vmem, hbm, hbm],
        out_specs=[hbm] * 5,
        scratch_shapes=[
            pltpu.VMEM((width, local), BF16),
            pltpu.VMEM((local, width), BF16),
            pltpu.VMEM((slots, nz, 2, rows, width), BF16),
            pltpu.VMEM((slots, chunks, nz, 2, rows, cols), BF16),
            pltpu.VMEM((slots, tokens, local), BF16),
            pltpu.VMEM((slots, tokens, local), BF16),
            pltpu.VMEM((tokens, local), F32),
            pltpu.VMEM((tokens, local), F32),
            pltpu.VMEM((chunks, nz, rows, cols), F32),
            pltpu.VMEM((slots, chunks, nz, rows, cols), BF16),
            pltpu.VMEM((slots, chunks, nz, rows, cols), BF16),
            pltpu.VMEM((slots, chunks, nz, rows, cols), BF16),
            pltpu.VMEM((slots, chunks, nz, rows, cols), BF16),
            pltpu.VMEM((slots, chunks, rows, cols), BF16),
            pltpu.VMEM((slots, 8, 128), F32),
            pltpu.VMEM((slots, parts, 8, 128), F32),
            pltpu.VMEM((slots, width, tokens), BF16),
            pltpu.VMEM((slots, tokens, width), BF16),
            dma((2, 4)),
            dma((2 * slots, nz)), dma((2 * slots, nz)), dma((2 * slots, nz)), dma((2 * slots, nz)),
            dma((slots, chunks)), dma((slots, chunks)),
            dma((slots, chunks, nz)), dma((slots, chunks, nz)),
            dma((slots - 1, chunks, nz)), dma((slots - 1, chunks, nz)),
            dma((slots - 1, chunks)), dma((slots - 1, chunks)),
            dma((slots, parts)), dma((slots, parts)),
            dma((slots, 4 + chunks)),
        ],
        compiler_params=pltpu.CompilerParams(collective_id=0, has_side_effects=True, vmem_limit_bytes=60 * 1024 * 1024),
        cost_estimate=pl.CostEstimate(flops=flops, bytes_accessed=4 * width * local, transcendentals=0),
        name="chain",
    )(slot_index, example_lengths, saved_inputs, first_grads, loss_grads, w_in, w_out)

    block = min(512, local)
    return pl.pallas_call(
        grads_kernel,
        grid=(local // block,),
        out_shape=(
            sds((1, width, local), BF16),
            sds((1, local, width), BF16),
            sds((1, slots, rows, width), BF16),
        ),
        in_specs=[
            pl.BlockSpec((slots, width, tokens), lambda i: (0, 0, 0)),
            pl.BlockSpec((slots, tokens, width), lambda i: (0, 0, 0)),
            pl.BlockSpec((slots, tokens, block), lambda i: (0, 0, i)),
            pl.BlockSpec((slots, tokens, block), lambda i: (0, 0, i)),
            pl.BlockSpec((slots, rows, width), lambda i: (0, 0, 0)),
        ],
        out_specs=[
            pl.BlockSpec((1, width, block), lambda i: (0, 0, i)),
            pl.BlockSpec((1, block, width), lambda i: (0, i, 0)),
            pl.BlockSpec((1, slots, rows, width), lambda i: (0, 0, 0, 0)),
        ],
        compiler_params=pltpu.CompilerParams(dimension_semantics=("arbitrary",), vmem_limit_bytes=60 * 1024 * 1024),
        cost_estimate=pl.CostEstimate(flops=4 * slots * tokens * width * local, bytes_accessed=8 * width * local, transcendentals=0),
        name="grads",
    )(xct, dyc, h, dz, res)


def shifted(value, axis, steps):
    count = lax.axis_size(axis)
    first, last = (max(0, -steps), min(count, count - steps))
    return lax.ppermute(value, axis, [(source, source + steps) for source in range(first, last)])


def membership(lengths, tokens):
    ends = jnp.cumsum(lengths)
    position = jnp.arange(tokens, dtype=jnp.int32)
    example_id = jnp.sum((position[:, None] >= ends[None, :-1]).astype(jnp.int32), axis=1)
    labels = jnp.arange(lengths.shape[0], dtype=jnp.int32)
    return (example_id[:, None] == labels[None, :]).astype(F32)


def spread(value, axis):
    copies = jnp.broadcast_to(value[None], (lax.axis_size(axis),) + value.shape)
    return lax.all_to_all(copies, axis, 0, 0)


def gram(value):
    return lax.dot_general(value, value, (((1,), (1,)), ((), ())), preferred_element_type=F32)


def per_device(saved_inputs, slot_index, example_lengths, first_grads, loss_grads, w_in, w_out):
    section_count = lax.axis_size("section")
    parts = lax.axis_size("tensor")
    is_last = lax.axis_index("section") == section_count - 1
    first = w_in[0]
    second = w_out[0]
    slot_count = loss_grads.shape[0] + 1
    rows, width = first_grads.shape[1:]
    hidden_all = first.shape[1] * parts
    picked = [
        lax.dynamic_index_in_dim(saved_inputs[0], slot_index[0, slot], 0, keepdims=False)
        for slot in range(slot_count)
    ]
    tokens = parts * rows
    opening = spread(jnp.concatenate([picked[0], first_grads[0]]), "tensor")
    later = spread(jnp.concatenate(picked[1:]), "tensor")
    every_input = [opening[:, :rows].reshape(tokens, width)]
    for slot in range(slot_count - 1):
        every_input.append(later[:, slot * rows : (slot + 1) * rows].reshape(tokens, width))
    incoming = first_grads[0]
    results, dzs, hiddens, grad_list, members, squares = [], [], [], [], [], []
    for slot in range(slot_count):
        inputs = every_input[slot]
        if slot == 0:
            grads = opening[:, rows:].reshape(tokens, width)
        else:
            grads = spread(incoming, "tensor").reshape(tokens, width)
        z = jnp.dot(inputs, first, preferred_element_type=F32)
        relu = jnp.maximum(z, 0.0)
        hidden = (relu * relu).astype(BF16)
        back = jnp.einsum("td,fd->tf", grads, second, preferred_element_type=F32)
        dz = (2.0 * relu * back).astype(BF16)
        own_terms = jnp.einsum("tf,df->td", dz, first, preferred_element_type=F32).astype(BF16)
        pieces = lax.all_to_all(own_terms.reshape(parts, rows, width), "tensor", 0, 0)
        shares = jnp.sum(pieces.astype(F32), axis=0)
        passing = (incoming.astype(F32) + shares).astype(BF16)
        results.append(passing)
        if slot + 1 < slot_count:
            arrived = shifted(passing, "section", -1)
            incoming = jnp.where(is_last, loss_grads[slot], arrived)
        member = membership(example_lengths[0, slot], inputs.shape[0])
        paired = gram(inputs) * gram(dz) + gram(hidden) * gram(grads)
        per_row = jnp.stack([jnp.sum(paired * member[:, e][None, :], axis=1) for e in range(member.shape[1])], axis=1)
        squares.append(jnp.sum(member * per_row, axis=0))
        dzs.append(dz)
        hiddens.append(hidden)
        grad_list.append(grads)
        members.append(member)
    local = jnp.stack(squares)
    total = jnp.sum(spread(local, "tensor"), axis=0)
    factor = 1.0 / (jnp.sqrt(total / (width * hidden_all)) + GAMMA)
    token_factor = jnp.concatenate([jnp.sum(m * factor[i][None, :], axis=1) for i, m in enumerate(members)])[:, None]
    xc = (jnp.concatenate(every_input).astype(F32) * token_factor).astype(BF16)
    dyc = (jnp.concatenate(grad_list).astype(F32) * token_factor).astype(BF16)
    grad_in = jnp.einsum("td,tf->df", xc, jnp.concatenate(dzs), preferred_element_type=F32).astype(BF16)[None]
    grad_out = jnp.einsum("tf,td->fd", jnp.concatenate(hiddens), dyc, preferred_element_type=F32).astype(BF16)[None]
    input_grads = jnp.stack(results)[None]
    return (grad_in, grad_out, input_grads)


def solution(mesh):
    sections = mesh.shape["section"]
    parts = mesh.shape["tensor"]

    def body(saved_inputs, slot_index, example_lengths, first_grads, loss_grads, w_in, w_out):
        rows, width = first_grads.shape[1:]
        fits = sections > 2 and parts % 2 == 0 and rows % 16 == 0 and width % 256 == 0 and w_in.shape[2] % 512 == 0 and loss_grads.shape[0] > 0
        run = functools.partial(fast_device, sections) if fits else per_device
        return run(saved_inputs, slot_index, example_lengths, first_grads, loss_grads, w_in, w_out)

    return jax.shard_map(
        body,
        mesh=mesh,
        in_specs=(
            P("section", None, "tensor", None),
            P("section", None),
            P("section", None, None),
            P("section", "tensor", None),
            P(None, "tensor", None),
            P("section", None, "tensor"),
            P("section", "tensor", None),
        ),
        out_specs=(
            P("section", None, "tensor"),
            P("section", "tensor", None),
            P("section", None, "tensor", None),
        ),
        check_vma=False,
    )
```

```python
import functools

import jax
import jax.numpy as jnp
from jax import lax
from jax.experimental import pallas as pl
from jax.experimental.pallas import tpu as pltpu
from jax.sharding import PartitionSpec as P

GAMMA = 0.01
F32 = jnp.float32
BF16 = jnp.bfloat16
MESH = pl.DeviceIdType.MESH
NT = (((1,), (1,)), ((), ()))
TN = (((0,), (0,)), ((), ()))


def dot(a, b, dims):
    return lax.dot_general(a, b, dims, preferred_element_type=F32)


def chain_kernel(
    cfg,
    index_ref, lengths_ref, saved_ref, first_ref, loss_ref, win_hbm, wout_hbm,
    gin_ref, gout_ref, res_ref,
    xg, dyb, h, dz, rbuf, acc, own, rxs, rxr, rzs, rzr, res, sqs, sqr, xct, dyc,
    w_sem, ag_send, ag_recv, fw_send, fw_recv, rx_send, rx_recv, rz_send, rz_recv,
    sh_send, sh_recv, af_send, af_recv, sq_send, sq_recv,
):
    sections, parts, nz, slots, rows, width, local, chunks, examples, hidden_all = cfg
    cols = width // chunks
    tokens = parts * rows
    win, wout = gin_ref.at[0], gout_ref.at[0]
    tile = min(2048, local)
    tiles = local // tile
    span = local // chunks
    s = lax.axis_index("section")
    p = lax.axis_index("tensor")
    z = p // 2
    x = p % 2
    is_last = s == sections - 1
    partner = {"section": s, "tensor": z * 2 + (1 - x)}

    def zpeer(j):
        return {"section": s, "tensor": ((z + j) % nz) * 2 + x}

    def behind(j):
        return {"section": s - 1, "tensor": ((z + j) % nz) * 2 + x}

    pieces = 4
    span_in, span_out = local // pieces, local // pieces
    for k in range(pieces):
        pltpu.make_async_copy(win_hbm.at[0, :, pl.ds(k * span_in, span_in)], win.at[:, pl.ds(k * span_in, span_in)], w_sem.at[0, k]).start()
    for k in range(pieces):
        pltpu.make_async_copy(wout_hbm.at[0, pl.ds(k * span_out, span_out)], wout.at[pl.ds(k * span_out, span_out)], w_sem.at[1, k]).start()

    for t in range(slots):
        xg[t, z, x] = saved_ref[0, index_ref[0, t]]
    for c in range(chunks):
        dyb[0, c, z, x] = first_ref[0, :, pl.ds(c * cols, cols)]

    @pl.when(is_last)
    def _():
        for t in range(1, slots):
            for c in range(chunks):
                dyb[t, c, z, x] = loss_ref[t - 1, :, pl.ds(c * cols, cols)]

    barrier = pltpu.get_barrier_semaphore()
    for j in range(1, parts):
        pl.semaphore_signal(barrier, inc=1, device_id={"section": s, "tensor": (p + j) % parts}, device_id_type=MESH)

    for side in (1, sections - 1):
        for j in range(nz):
            pl.semaphore_signal(barrier, inc=1, device_id={"section": (s + side) % sections, "tensor": ((z + j) % nz) * 2 + x}, device_id_type=MESH)
    pl.semaphore_wait(barrier, parts - 1 + 2 * nz)

    def block(k, source):
        if k < slots:
            return xg.at[k, source, x]
        return dyb.at[k - slots, :, source, x]

    def ag_copy(k, j, to_partner):
        if to_partner:
            ref = block(k, (z + nz - j) % nz)
            return pltpu.make_async_remote_copy(ref, ref, fw_send.at[k, j], fw_recv.at[k, j], device_id=partner, device_id_type=MESH)
        ref = block(k, z)
        return pltpu.make_async_remote_copy(ref, ref, ag_send.at[k, j], ag_recv.at[k, j], device_id=zpeer(j), device_id_type=MESH)

    def ag_open(k):
        for j in range(1, nz):
            ag_copy(k, j, False).start()

    def ag_forward(k):
        ag_copy(k, 0, True).start()
        for j in range(1, nz):
            ag_copy(k, j, False).wait_recv()
            ag_copy(k, j, True).start()

    def ag_finish(k):
        for j in range(nz):
            ag_copy(k, j, True).wait_recv()

    def ag_drain(k):
        for j in range(nz):
            if j:
                ag_copy(k, j, False).wait_send()
            ag_copy(k, j, True).wait_send()

    def z_tiles(t, lo, hi):
        def body(i, carry):
            at = pl.ds(pl.multiple_of(i * tile, tile), tile)
            zz = jnp.dot(xg[t].reshape(tokens, width), win[:, at], preferred_element_type=F32)
            r = jnp.maximum(zz, 0.0)
            rbuf[:, at] = r
            h[t, :, at] = (r * r).astype(BF16)
            return carry

        lax.fori_loop(lo, hi, body, 0)

    def back_all(t):
        def body(i, carry):
            at = pl.ds(pl.multiple_of(i * tile, tile), tile)
            grads = jnp.concatenate([dyb[t, c].reshape(tokens, cols) for c in range(chunks)], axis=1)
            dh = dot(grads, wout[at, :], NT)
            dz[t, :, at] = (2.0 * rbuf[:, at] * dh).astype(BF16)
            return carry

        lax.fori_loop(0, tiles, body, 0)

    def back_chunk(t, c, mode):
        def body(i, carry):
            at = pl.ds(pl.multiple_of(i * tile, tile), tile)
            dh = dot(dyb[t, c].reshape(tokens, cols), wout[at, c * cols:(c + 1) * cols], NT)
            if mode > 0:
                dh = dh + acc[:, at]
            if mode < 2:
                acc[:, at] = dh
            else:
                dz[t, :, at] = (2.0 * rbuf[:, at] * dh).astype(BF16)
            return carry

        lax.fori_loop(0, tiles, body, 0)

    def rx_copy(t, c):
        return pltpu.make_async_remote_copy(rxs.at[t, c], rxr.at[t, c], rx_send.at[t, c], rx_recv.at[t, c], device_id=partner, device_id_type=MESH)

    def rz_copy(t, c, j):
        return pltpu.make_async_remote_copy(rzs.at[t, c, (z + j) % nz], rzr.at[t, c, j], rz_send.at[t, c, j], rz_recv.at[t, c, j], device_id=zpeer(j), device_id_type=MESH)

    def sh_copy(t, c, j):
        return pltpu.make_async_remote_copy(res.at[t, c], dyb.at[t + 1, c, z, x], sh_send.at[t, c, j], sh_recv.at[t, c, j], device_id=behind(j), device_id_type=MESH)

    def af_copy(t, c):
        ref = dyb.at[t + 1, c, :, x]
        return pltpu.make_async_remote_copy(ref, ref, af_send.at[t, c], af_recv.at[t, c], device_id=partner, device_id_type=MESH)

    def over_chunks(body):
        def step(c, carry):
            body(c)
            return carry

        lax.fori_loop(0, chunks, step, 0)

    def partial_dx(t):
        def body(c):
            wide = win[pl.ds(pl.multiple_of(c * cols, cols), cols), :]
            part = dot(dz[t], wide, NT).reshape(nz, 2, rows, cols)
            first_half, second_half = part[:, 0], part[:, 1]
            mine = jnp.where(x == 0, first_half, second_half)
            other = jnp.where(x == 0, second_half, first_half)
            own[c] = mine
            rxs[t, c] = other.astype(BF16)
            rx_copy(t, c).start()

        over_chunks(body)

    def pair_sum(t, c):
        rx_copy(t, c).wait_recv()
        total = own[c] + rxr[t, c].astype(F32)
        own[c] = total
        rzs[t, c] = total.astype(BF16)
        for j in range(1, nz):
            rz_copy(t, c, j).start()

    def line_sum(t, c):
        total = own[c, z] + dyb[t, c, z, x].astype(F32)
        for j in range(1, nz):
            rz_copy(t, c, j).wait_recv()
            total = total + rzr[t, c, j].astype(F32)
        res[t, c] = total.astype(BF16)
        if t + 1 < slots:
            @pl.when(s > 0)
            def _():
                for j in range(nz):
                    sh_copy(t, c, j).start()

    def hand_over(t, c):
        for j in range(nz):
            sh_copy(t, c, j).wait_recv()
        af_copy(t, c).start()

    def example_mask(t):
        position = lax.broadcasted_iota(jnp.int32, (tokens, 1), 0)
        across = lax.broadcasted_iota(jnp.int32, (1, tokens), 1)
        down, along = [], []
        start = jnp.int32(0)
        for e in range(examples):
            stop = start + lengths_ref[0, e, t]
            if e == examples - 1:
                stop = jnp.int32(tokens)
            down.append((position >= start) & (position < stop))
            along.append((across >= start) & (across < stop))
            start = stop
        return down, along

    def sq_copy(t, j):
        return pltpu.make_async_remote_copy(sqs.at[t], sqr.at[t, j], sq_send.at[t, j], sq_recv.at[t, j], device_id={"section": s, "tensor": (p + j) % parts}, device_id_type=MESH)

    def squares(t):
        inputs = xg[t].reshape(tokens, width)
        grads = jnp.concatenate([dyb[t, c].reshape(tokens, cols) for c in range(chunks)], axis=1)
        paired = dot(inputs, inputs, NT) * dot(dz[t], dz[t], NT) + dot(h[t], h[t], NT) * dot(grads, grads, NT)
        down, along = example_mask(t)
        row = lax.broadcasted_iota(jnp.int32, (8, 128), 0)
        out = jnp.zeros((8, 128), F32)
        for e in range(examples):
            kept = jnp.where(down[e], paired, 0.0)
            kept = jnp.where(along[e], kept, 0.0)
            value = jnp.sum(jnp.sum(kept, axis=0, keepdims=True), axis=1, keepdims=True)
            out = jnp.where(row == e, value, out)
        sqs[t] = out
        for j in range(1, parts):
            sq_copy(t, j).start()

    def scale(t):
        total = sqs[t]
        for j in range(1, parts):
            sq_copy(t, j).wait_recv()
            total = total + sqr[t, j]
        factor = 1.0 / (jnp.sqrt(total / (width * hidden_all)) + GAMMA)
        down, _ = example_mask(t)
        per_token = jnp.zeros((tokens, 1), F32)
        for e in range(examples):
            per_token = jnp.where(down[e], factor[e:e + 1, 0:1], per_token)
        scaled = xg[t].reshape(tokens, width).astype(F32) * per_token
        xct[t] = scaled.T.astype(BF16)
        for c in range(chunks):
            dyc[t, :, pl.ds(c * cols, cols)] = (dyb[t, c].reshape(tokens, cols).astype(F32) * per_token).astype(BF16)

    def grad_in_block(i):
        at = pl.ds(pl.multiple_of(i * span, span), span)
        lhs = jnp.concatenate([xct[t] for t in range(slots)], axis=1)
        rhs = jnp.concatenate([dz[t, :, at] for t in range(slots)], axis=0)
        win[:, at] = jnp.dot(lhs, rhs, preferred_element_type=F32).astype(BF16)

    def grad_out_block(i):
        at = pl.ds(pl.multiple_of(i * span, span), span)
        lhs = jnp.concatenate([h[t, :, at] for t in range(slots)], axis=0)
        wout[at, :] = dot(lhs, dyc[...].reshape(slots * tokens, width), TN).astype(BF16)

    ag_open(0)
    ag_open(slots)
    ag_open(1)

    @pl.when(is_last)
    def _():
        ag_open(slots + 1)

    for t in range(2, slots):
        ag_open(t)

    @pl.when(is_last)
    def _():
        for t in range(2, slots):
            ag_open(slots + t)

    ag_forward(0)
    ag_forward(slots)
    for k in range(pieces):
        pltpu.make_async_copy(win_hbm.at[0, :, pl.ds(k * span_in, span_in)], win.at[:, pl.ds(k * span_in, span_in)], w_sem.at[0, k]).wait()
    for k in range(pieces):
        pltpu.make_async_copy(wout_hbm.at[0, pl.ds(k * span_out, span_out)], wout.at[pl.ds(k * span_out, span_out)], w_sem.at[1, k]).wait()
    ag_finish(0)
    z_tiles(0, 0, tiles)
    ag_finish(slots)
    back_all(0)

    for t in range(slots - 1):
        partial_dx(t)
        squares(t)
        ag_forward(t + 1)

        @pl.when(is_last)
        def _():
            ag_forward(slots + t + 1)

        over_chunks(lambda c: pair_sum(t, c))
        ag_finish(t + 1)
        z_tiles(t + 1, 0, tiles)
        scale(t)
        over_chunks(lambda c: line_sum(t, c))

        @pl.when(s < sections - 1)
        def _():
            over_chunks(lambda c: hand_over(t, c))

        @pl.when(is_last)
        def _():
            ag_finish(slots + t + 1)

        for c in range(chunks):
            @pl.when(s < sections - 1)
            def _():
                af_copy(t, c).wait_recv()

            back_chunk(t + 1, c, 0 if c == 0 else (2 if c == chunks - 1 else 1))

    end = slots - 1
    squares(end)
    partial_dx(end)
    scale(end)

    def first_half(c):
        pair_sum(end, c)
        grad_in_block(c)

    def second_half(c):
        grad_out_block(c)
        line_sum(end, c)

    over_chunks(first_half)
    over_chunks(second_half)

    for t in range(slots):
        for c in range(chunks):
            res_ref[0, t, :, c * cols:(c + 1) * cols] = res[t, c]

    for t in range(slots):
        ag_drain(t)
    ag_drain(slots)

    @pl.when(is_last)
    def _():
        for t in range(1, slots):
            ag_drain(slots + t)

    for t in range(slots):
        def drain(c):
            rx_copy(t, c).wait_send()
            for j in range(1, nz):
                rz_copy(t, c, j).wait_send()

        over_chunks(drain)
        for j in range(1, parts):
            sq_copy(t, j).wait_send()
        if t + 1 < slots:
            @pl.when(s > 0)
            def _():
                def drain_shift(c):
                    for j in range(nz):
                        sh_copy(t, c, j).wait_send()

                over_chunks(drain_shift)

            @pl.when(s < sections - 1)
            def _():
                over_chunks(lambda c: af_copy(t, c).wait_send())


FLUSH = 4


def flush_kernel(gin_ref, gout_ref, res_ref, gin_hbm, gout_hbm, res_hbm, sem):
    copies = []
    for k, (source, target) in enumerate(((gin_ref, gin_hbm), (gout_ref, gout_hbm))):
        step = source.shape[1] // FLUSH
        for i in range(FLUSH):
            at = pl.ds(i * step, step)
            copies.append(pltpu.make_async_copy(source.at[:, at], target.at[:, at], sem.at[k * FLUSH + i]))
    copies.append(pltpu.make_async_copy(res_ref, res_hbm, sem.at[2 * FLUSH]))
    for copy in copies:
        copy.start()
    for copy in copies:
        copy.wait()


def fast_device(sections, saved_inputs, slot_index, example_lengths, first_grads, loss_grads, w_in, w_out):
    parts = lax.axis_size("tensor")
    slots = loss_grads.shape[0] + 1
    rows, width = first_grads.shape[1:]
    local = w_in.shape[2]
    nz = parts // 2
    tokens = parts * rows
    examples = example_lengths.shape[2]
    chunks = max(1, width // 256)
    cols = width // chunks
    cfg = (sections, parts, nz, slots, rows, width, local, chunks, examples, local * parts)
    hbm = pl.BlockSpec(memory_space=pl.ANY)
    vmem = pl.BlockSpec(memory_space=pltpu.VMEM)
    smem = pl.BlockSpec(memory_space=pltpu.SMEM)
    dma = pltpu.SemaphoreType.DMA
    sds = jax.ShapeDtypeStruct
    flops = 2 * tokens * width * local * slots * 5
    grad_in, grad_out, results = pl.pallas_call(
        functools.partial(chain_kernel, cfg),
        out_shape=(
            pltpu.VMEM((1, width, local), BF16),
            pltpu.VMEM((1, local, width), BF16),
            pltpu.VMEM((1, slots, rows, width), BF16),
        ),
        in_specs=[smem, smem, vmem, vmem, vmem, hbm, hbm],
        out_specs=[vmem, vmem, vmem],
        scratch_shapes=[
            pltpu.VMEM((slots, nz, 2, rows, width), BF16),
            pltpu.VMEM((slots, chunks, nz, 2, rows, cols), BF16),
            pltpu.VMEM((slots, tokens, local), BF16),
            pltpu.VMEM((slots, tokens, local), BF16),
            pltpu.VMEM((tokens, local), F32),
            pltpu.VMEM((tokens, local), F32),
            pltpu.VMEM((chunks, nz, rows, cols), F32),
            pltpu.VMEM((slots, chunks, nz, rows, cols), BF16),
            pltpu.VMEM((slots, chunks, nz, rows, cols), BF16),
            pltpu.VMEM((slots, chunks, nz, rows, cols), BF16),
            pltpu.VMEM((slots, chunks, nz, rows, cols), BF16),
            pltpu.VMEM((slots, chunks, rows, cols), BF16),
            pltpu.VMEM((slots, 8, 128), F32),
            pltpu.VMEM((slots, parts, 8, 128), F32),
            pltpu.VMEM((slots, width, tokens), BF16),
            pltpu.VMEM((slots, tokens, width), BF16),
            dma((2, 4)),
            dma((2 * slots, nz)), dma((2 * slots, nz)), dma((2 * slots, nz)), dma((2 * slots, nz)),
            dma((slots, chunks)), dma((slots, chunks)),
            dma((slots, chunks, nz)), dma((slots, chunks, nz)),
            dma((slots - 1, chunks, nz)), dma((slots - 1, chunks, nz)),
            dma((slots - 1, chunks)), dma((slots - 1, chunks)),
            dma((slots, parts)), dma((slots, parts)),
        ],
        compiler_params=pltpu.CompilerParams(collective_id=0, has_side_effects=True, vmem_limit_bytes=44 * 1024 * 1024),
        cost_estimate=pl.CostEstimate(flops=flops, bytes_accessed=4 * width * local, transcendentals=0),
        name="chain",
    )(slot_index, jnp.swapaxes(example_lengths, 1, 2), saved_inputs, first_grads, loss_grads, w_in, w_out)

    return pl.pallas_call(
        flush_kernel,
        out_shape=(
            sds((1, width, local), BF16),
            sds((1, local, width), BF16),
            sds((1, slots, rows, width), BF16),
        ),
        in_specs=[vmem] * 3,
        out_specs=[hbm] * 3,
        scratch_shapes=[dma((FLUSH * 2 + 1,))],
        compiler_params=pltpu.CompilerParams(vmem_limit_bytes=1024 * 1024),
        cost_estimate=pl.CostEstimate(flops=0, bytes_accessed=8 * width * local, transcendentals=0),
        name="flush",
    )(grad_in, grad_out, results)


def shifted(value, axis, steps):
    count = lax.axis_size(axis)
    first, last = (max(0, -steps), min(count, count - steps))
    return lax.ppermute(value, axis, [(source, source + steps) for source in range(first, last)])


def membership(lengths, tokens):
    ends = jnp.cumsum(lengths)
    position = jnp.arange(tokens, dtype=jnp.int32)
    example_id = jnp.sum((position[:, None] >= ends[None, :-1]).astype(jnp.int32), axis=1)
    labels = jnp.arange(lengths.shape[0], dtype=jnp.int32)
    return (example_id[:, None] == labels[None, :]).astype(F32)


def spread(value, axis):
    copies = jnp.broadcast_to(value[None], (lax.axis_size(axis),) + value.shape)
    return lax.all_to_all(copies, axis, 0, 0)


def gram(value):
    return lax.dot_general(value, value, (((1,), (1,)), ((), ())), preferred_element_type=F32)


def per_device(saved_inputs, slot_index, example_lengths, first_grads, loss_grads, w_in, w_out):
    section_count = lax.axis_size("section")
    parts = lax.axis_size("tensor")
    is_last = lax.axis_index("section") == section_count - 1
    first = w_in[0]
    second = w_out[0]
    slot_count = loss_grads.shape[0] + 1
    rows, width = first_grads.shape[1:]
    hidden_all = first.shape[1] * parts
    picked = [
        lax.dynamic_index_in_dim(saved_inputs[0], slot_index[0, slot], 0, keepdims=False)
        for slot in range(slot_count)
    ]
    tokens = parts * rows
    opening = spread(jnp.concatenate([picked[0], first_grads[0]]), "tensor")
    later = spread(jnp.concatenate(picked[1:]), "tensor")
    every_input = [opening[:, :rows].reshape(tokens, width)]
    for slot in range(slot_count - 1):
        every_input.append(later[:, slot * rows : (slot + 1) * rows].reshape(tokens, width))
    incoming = first_grads[0]
    results, dzs, hiddens, grad_list, members, squares = [], [], [], [], [], []
    for slot in range(slot_count):
        inputs = every_input[slot]
        if slot == 0:
            grads = opening[:, rows:].reshape(tokens, width)
        else:
            grads = spread(incoming, "tensor").reshape(tokens, width)
        z = jnp.dot(inputs, first, preferred_element_type=F32)
        relu = jnp.maximum(z, 0.0)
        hidden = (relu * relu).astype(BF16)
        back = jnp.einsum("td,fd->tf", grads, second, preferred_element_type=F32)
        dz = (2.0 * relu * back).astype(BF16)
        own_terms = jnp.einsum("tf,df->td", dz, first, preferred_element_type=F32).astype(BF16)
        pieces = lax.all_to_all(own_terms.reshape(parts, rows, width), "tensor", 0, 0)
        shares = jnp.sum(pieces.astype(F32), axis=0)
        passing = (incoming.astype(F32) + shares).astype(BF16)
        results.append(passing)
        if slot + 1 < slot_count:
            arrived = shifted(passing, "section", -1)
            incoming = jnp.where(is_last, loss_grads[slot], arrived)
        member = membership(example_lengths[0, slot], inputs.shape[0])
        paired = gram(inputs) * gram(dz) + gram(hidden) * gram(grads)
        per_row = jnp.stack([jnp.sum(paired * member[:, e][None, :], axis=1) for e in range(member.shape[1])], axis=1)
        squares.append(jnp.sum(member * per_row, axis=0))
        dzs.append(dz)
        hiddens.append(hidden)
        grad_list.append(grads)
        members.append(member)
    local = jnp.stack(squares)
    total = jnp.sum(spread(local, "tensor"), axis=0)
    factor = 1.0 / (jnp.sqrt(total / (width * hidden_all)) + GAMMA)
    token_factor = jnp.concatenate([jnp.sum(m * factor[i][None, :], axis=1) for i, m in enumerate(members)])[:, None]
    xc = (jnp.concatenate(every_input).astype(F32) * token_factor).astype(BF16)
    dyc = (jnp.concatenate(grad_list).astype(F32) * token_factor).astype(BF16)
    grad_in = jnp.einsum("td,tf->df", xc, jnp.concatenate(dzs), preferred_element_type=F32).astype(BF16)[None]
    grad_out = jnp.einsum("tf,td->fd", jnp.concatenate(hiddens), dyc, preferred_element_type=F32).astype(BF16)[None]
    input_grads = jnp.stack(results)[None]
    return (grad_in, grad_out, input_grads)


def solution(mesh):
    sections = mesh.shape["section"]
    parts = mesh.shape["tensor"]

    def body(saved_inputs, slot_index, example_lengths, first_grads, loss_grads, w_in, w_out):
        rows, width = first_grads.shape[1:]
        fits = sections > 2 and parts % 2 == 0 and rows % 16 == 0 and width % 256 == 0 and w_in.shape[2] % 512 == 0 and loss_grads.shape[0] > 0
        run = functools.partial(fast_device, sections) if fits else per_device
        return run(saved_inputs, slot_index, example_lengths, first_grads, loss_grads, w_in, w_out)

    return jax.shard_map(
        body,
        mesh=mesh,
        in_specs=(
            P("section", None, "tensor", None),
            P("section", None),
            P("section", None, None),
            P("section", "tensor", None),
            P(None, "tensor", None),
            P("section", None, "tensor"),
            P("section", "tensor", None),
        ),
        out_specs=(
            P("section", None, "tensor"),
            P("section", "tensor", None),
            P("section", None, "tensor", None),
        ),
        check_vma=False,
    )
```

```python
import functools

import jax
import jax.numpy as jnp
from jax import lax
from jax.experimental import pallas as pl
from jax.experimental.pallas import tpu as pltpu
from jax.sharding import PartitionSpec as P

GAMMA = 0.01
F32 = jnp.float32
BF16 = jnp.bfloat16
MESH = pl.DeviceIdType.MESH
NT = (((1,), (1,)), ((), ()))
TN = (((0,), (0,)), ((), ()))


def dot(a, b, dims):
    return lax.dot_general(a, b, dims, preferred_element_type=F32)


def chain_kernel(
    cfg,
    index_hbm, lengths_hbm, saved_hbm, first_hbm, loss_hbm, win_hbm, wout_hbm,
    gin_ref, gout_ref, h, dyc, res_ref,
    xg, dyb, dz, rbuf, acc, gxs, ghs, own, rxs, rxr, rzs, rzr, res, sqs, sqr, xct,
    index_ref, lengths_ref, saved_ref, in_sem,
    w_sem, ag_send, ag_recv, fw_send, fw_recv, rx_send, rx_recv, rz_send, rz_recv,
    sh_send, sh_recv, af_send, af_recv, sq_send, sq_recv,
):
    sections, parts, nz, slots, rows, width, local, chunks, sub, ready, examples, hidden_all = cfg
    cols = width // chunks
    count = chunks * sub
    part_cols = cols // sub
    tokens = parts * rows
    win, wout = gin_ref.at[0], gout_ref.at[0]
    span = local // chunks
    s = lax.axis_index("section")
    p = lax.axis_index("tensor")
    z = p // 2
    x = p % 2
    is_last = s == sections - 1
    partner = {"section": s, "tensor": z * 2 + (1 - x)}

    def zpeer(j):
        return {"section": s, "tensor": ((z + j) % nz) * 2 + x}

    def behind(j):
        return {"section": s - 1, "tensor": ((z + j) % nz) * 2 + x}

    index_in = pltpu.make_async_copy(index_hbm, index_ref, in_sem.at[0])
    lengths_in = pltpu.make_async_copy(lengths_hbm, lengths_ref, in_sem.at[1])
    saved_in = pltpu.make_async_copy(saved_hbm.at[0], saved_ref, in_sem.at[2])
    index_in.start()
    saved_in.start()
    lengths_in.start()

    def grads_in(t, c):
        source = first_hbm.at[0] if t == 0 else loss_hbm.at[t - 1]
        return pltpu.make_async_copy(source.at[:, c * part_cols:(c + 1) * part_cols], dyb.at[t, c, z, x], in_sem.at[3 + t * count + c])

    for c in range(count):
        grads_in(0, c).start()

    @pl.when(is_last)
    def _():
        for t in range(1, slots):
            for c in range(count):
                grads_in(t, c).start()

    pieces = 4
    span_in, span_out = local // pieces, local // pieces
    for k in range(pieces):
        pltpu.make_async_copy(win_hbm.at[0, :, pl.ds(k * span_in, span_in)], win.at[:, pl.ds(k * span_in, span_in)], w_sem.at[0, k]).start()
    for k in range(pieces):
        pltpu.make_async_copy(wout_hbm.at[0, pl.ds(k * span_out, span_out)], wout.at[pl.ds(k * span_out, span_out)], w_sem.at[1, k]).start()

    barrier = pltpu.get_barrier_semaphore()
    for j in range(1, parts):
        pl.semaphore_signal(barrier, inc=1, device_id={"section": s, "tensor": (p + j) % parts}, device_id_type=MESH)

    for side in (1, sections - 1):
        for j in range(nz):
            pl.semaphore_signal(barrier, inc=1, device_id={"section": (s + side) % sections, "tensor": ((z + j) % nz) * 2 + x}, device_id_type=MESH)
    index_in.wait()
    saved_in.wait()
    for t in range(slots):
        xg[t, z, x] = saved_ref[index_ref[0, t]]
    for c in range(count):
        grads_in(0, c).wait()
    lengths_in.wait()

    @pl.when(is_last)
    def _():
        for t in range(1, slots):
            for c in range(count):
                grads_in(t, c).wait()

    pl.semaphore_wait(barrier, parts - 1 + 2 * nz)

    def block(k, source):
        if k < slots:
            return xg.at[k, source, x]
        return dyb.at[k - slots, :, source, x]

    def ag_copy(k, j, to_partner):
        if to_partner:
            ref = block(k, (z + nz - j) % nz)
            return pltpu.make_async_remote_copy(ref, ref, fw_send.at[k, j], fw_recv.at[k, j], device_id=partner, device_id_type=MESH)
        ref = block(k, z)
        return pltpu.make_async_remote_copy(ref, ref, ag_send.at[k, j], ag_recv.at[k, j], device_id=zpeer(j), device_id_type=MESH)

    def ag_open(k):
        for j in range(1, nz):
            ag_copy(k, j, False).start()

    def ag_forward(k):
        ag_copy(k, 0, True).start()
        for j in range(1, nz):
            ag_copy(k, j, False).wait_recv()
            ag_copy(k, j, True).start()

    def ag_finish(k):
        for j in range(nz):
            ag_copy(k, j, True).wait_recv()

    def ag_drain(k):
        for j in range(nz):
            if j:
                ag_copy(k, j, False).wait_send()
            ag_copy(k, j, True).wait_send()

    def grads_of(t, lo, hi):
        return jnp.concatenate([dyb[t, c].reshape(tokens, part_cols) for c in range(lo, hi)], axis=1)

    def z_tile(t, i, size):
        at = pl.ds(pl.multiple_of(i * size, size), size)
        zz = jnp.dot(xg[t].reshape(tokens, width), win[:, at], preferred_element_type=F32)
        r = jnp.maximum(zz, 0.0)
        rbuf[:, at] = r
        h[t, :, at] = (r * r).astype(BF16)

    def back_tile(t, i, size):
        at = pl.ds(pl.multiple_of(i * size, size), size)
        dh = dot(grads_of(t, 0, count), wout[at, :], NT)
        dz[t, :, at] = (2.0 * rbuf[:, at] * dh).astype(BF16)

    def back_chunk(t, c, mode):
        size = min(2048, local)

        def body(i, carry):
            at = pl.ds(pl.multiple_of(i * size, size), size)
            dh = dot(grads_of(t, c * sub, (c + 1) * sub), wout[at, c * cols:(c + 1) * cols], NT)
            if mode > 0:
                dh = dh + acc[:, at]
            if mode < 2:
                acc[:, at] = dh
            else:
                dz[t, :, at] = (2.0 * rbuf[:, at] * dh).astype(BF16)
            return carry

        lax.fori_loop(0, local // size, body, 0)

    def rx_copy(t, c):
        return pltpu.make_async_remote_copy(rxs.at[t, c], rxr.at[t, c], rx_send.at[t, c], rx_recv.at[t, c], device_id=partner, device_id_type=MESH)

    def rz_copy(t, c, j):
        return pltpu.make_async_remote_copy(rzs.at[t, c, (z + j) % nz], rzr.at[t, c, j], rz_send.at[t, c, j], rz_recv.at[t, c, j], device_id=zpeer(j), device_id_type=MESH)

    def sh_copy(t, c, j):
        return pltpu.make_async_remote_copy(res.at[t, c], dyb.at[t + 1, c, z, x], sh_send.at[t, c, j], sh_recv.at[t, c, j], device_id=behind(j), device_id_type=MESH)

    def af_copy(t, c):
        ref = dyb.at[t + 1, c, :, x]
        return pltpu.make_async_remote_copy(ref, ref, af_send.at[t, c], af_recv.at[t, c], device_id=partner, device_id_type=MESH)

    def over(lo, hi, body):
        def step(c, carry):
            body(c)
            return carry

        lax.fori_loop(lo, hi, step, 0)

    def partial_dx(t):
        def body(c):
            wide = win[pl.ds(pl.multiple_of(c * cols, cols), cols), :]
            whole = dot(dz[t], wide, NT)
            for u in range(sub):
                part = whole[:, u * part_cols:(u + 1) * part_cols].reshape(nz, 2, rows, part_cols)
                first_half, second_half = part[:, 0], part[:, 1]
                mine = jnp.where(x == 0, first_half, second_half)
                other = jnp.where(x == 0, second_half, first_half)
                own[c * sub + u] = mine
                rxs[t, c * sub + u] = other.astype(BF16)
                rx_copy(t, c * sub + u).start()

        over(0, chunks, body)

    def pair_sum(t, c):
        rx_copy(t, c).wait_recv()
        total = own[c] + rxr[t, c].astype(F32)
        own[c] = total
        rzs[t, c] = total.astype(BF16)
        for j in range(1, nz):
            rz_copy(t, c, j).start()

    def line_sum(t, c):
        total = own[c, z] + dyb[t, c, z, x].astype(F32)
        for j in range(1, nz):
            rz_copy(t, c, j).wait_recv()
            total = total + rzr[t, c, j].astype(F32)
        res[t, c] = total.astype(BF16)
        if t + 1 < slots:
            @pl.when(s > 0)
            def _():
                for j in range(nz):
                    sh_copy(t, c, j).start()

    def hand_over(t, c):
        for j in range(nz):
            sh_copy(t, c, j).wait_recv()
        af_copy(t, c).start()

    def example_mask(t):
        position = lax.broadcasted_iota(jnp.int32, (tokens, 1), 0)
        across = lax.broadcasted_iota(jnp.int32, (1, tokens), 1)
        down, along = [], []
        start = jnp.int32(0)
        for e in range(examples):
            stop = start + lengths_ref[0, e, t]
            if e == examples - 1:
                stop = jnp.int32(tokens)
            down.append((position >= start) & (position < stop))
            along.append((across >= start) & (across < stop))
            start = stop
        return down, along

    def sq_copy(t, j):
        return pltpu.make_async_remote_copy(sqs.at[t], sqr.at[t, j], sq_send.at[t, j], sq_recv.at[t, j], device_id={"section": s, "tensor": (p + j) % parts}, device_id_type=MESH)

    def grams(t):
        inputs = xg[t].reshape(tokens, width)
        gxs[...] = dot(inputs, inputs, NT)
        ghs[...] = dot(h[t], h[t], NT)

    def squares(t):
        grads = grads_of(t, 0, count)
        paired = gxs[...] * dot(dz[t], dz[t], NT) + ghs[...] * dot(grads, grads, NT)
        down, along = example_mask(t)
        row = lax.broadcasted_iota(jnp.int32, (8, 128), 0)
        out = jnp.zeros((8, 128), F32)
        for e in range(examples):
            kept = jnp.where(down[e], paired, 0.0)
            kept = jnp.where(along[e], kept, 0.0)
            value = jnp.sum(jnp.sum(kept, axis=0, keepdims=True), axis=1, keepdims=True)
            out = jnp.where(row == e, value, out)
        sqs[t] = out
        for j in range(1, parts):
            sq_copy(t, j).start()

    def factors(t):
        total = sqs[t]
        for j in range(1, parts):
            sq_copy(t, j).wait_recv()
            total = total + sqr[t, j]
        factor = 1.0 / (jnp.sqrt(total / (width * hidden_all)) + GAMMA)
        down, _ = example_mask(t)
        per_token = jnp.zeros((tokens, 1), F32)
        for e in range(examples):
            per_token = jnp.where(down[e], factor[e:e + 1, 0:1], per_token)
        return per_token

    def scale(t, k, per_token):
        at = slice(k * part_cols, (k + 1) * part_cols)
        scaled = xg[t, :, :, :, at].reshape(tokens, part_cols).astype(F32) * per_token
        xct[t, at] = scaled.T.astype(BF16)
        dyc[t, :, at] = (dyb[t, k].reshape(tokens, part_cols).astype(F32) * per_token).astype(BF16)

    def grad_in_block(i):
        at = pl.ds(i * span, span)
        lhs = jnp.concatenate([xct[t] for t in range(slots)], axis=1)
        rhs = jnp.concatenate([dz[t, :, at] for t in range(slots)], axis=0)
        win[:, at] = jnp.dot(lhs, rhs, preferred_element_type=F32).astype(BF16)

    def grad_out_block(i):
        at = pl.ds(i * span, span)
        lhs = jnp.concatenate([h[t, :, at] for t in range(slots)], axis=0)
        wout[at, :] = dot(lhs, dyc[...].reshape(slots * tokens, width), TN).astype(BF16)

    end = slots - 1
    ag_open(0)
    ag_open(slots)
    if end > 0:
        ag_open(1)

        @pl.when(is_last)
        def _():
            ag_open(slots + 1)

    ag_forward(0)
    ag_forward(slots)
    for k in range(pieces):
        pltpu.make_async_copy(win_hbm.at[0, :, pl.ds(k * span_in, span_in)], win.at[:, pl.ds(k * span_in, span_in)], w_sem.at[0, k]).wait()
    ag_finish(0)
    over(0, 2, lambda i: z_tile(0, i, local // 2))
    grams(0)
    for k in range(pieces):
        pltpu.make_async_copy(wout_hbm.at[0, pl.ds(k * span_out, span_out)], wout.at[pl.ds(k * span_out, span_out)], w_sem.at[1, k]).wait()
    ag_finish(slots)
    over(0, 2, lambda i: back_tile(0, i, local // 2))

    for t in range(end):
        partial_dx(t)
        ag_forward(t + 1)
        if t > 0:
            grams(t)
        squares(t)
        over(0, count, lambda k: pair_sum(t, k))

        @pl.when(is_last)
        def _():
            ag_forward(slots + t + 1)

        per_token = None
        for k in range(count):
            line_sum(t, k)
            if k == 1:
                per_token = factors(t)
            if k > 1:
                scale(t, k - 2, per_token)
        if t + 2 < slots:
            ag_open(t + 2)

            @pl.when(is_last)
            def _():
                ag_open(slots + t + 2)

        for k in range(count - 2, count):
            scale(t, k, per_token)
        ag_finish(t + 1)

        def tile_and_hand(c):
            @pl.when(s < sections - 1)
            def _():
                for u in range(sub):
                    hand_over(t, c * sub + u)

            z_tile(t + 1, c, span)

        over(0, chunks, tile_and_hand)
        if t + 1 == end:
            grams(end)

        @pl.when(is_last)
        def _():
            ag_finish(slots + t + 1)

        for c in range(chunks):
            @pl.when(s < sections - 1)
            def _():
                for u in range(sub):
                    af_copy(t, c * sub + u).wait_recv()

            back_chunk(t + 1, c, 0 if c == 0 else (2 if c == chunks - 1 else 1))

    squares(end)
    partial_dx(end)
    per_token = factors(end)
    for k in range(count):
        scale(end, k, per_token)
    for c in range(chunks):
        for k in range(count):
            if min(chunks - 1, (k + 2) // 3) == c:
                pair_sum(end, k)
        grad_in_block(c)
    for i in range(ready):
        grad_out_block(i)
    over(0, count, lambda k: line_sum(end, k))

    for t in range(slots):
        for c in range(count):
            res_ref[0, t, :, c * part_cols:(c + 1) * part_cols] = res[t, c]

    for t in range(slots):
        ag_drain(t)
    ag_drain(slots)

    @pl.when(is_last)
    def _():
        for t in range(1, slots):
            ag_drain(slots + t)

    for t in range(slots):
        def drain(c):
            rx_copy(t, c).wait_send()
            for j in range(1, nz):
                rz_copy(t, c, j).wait_send()

        over(0, count, drain)
        for j in range(1, parts):
            sq_copy(t, j).wait_send()
        if t + 1 < slots:
            @pl.when(s > 0)
            def _():
                def drain_shift(c):
                    for j in range(nz):
                        sh_copy(t, c, j).wait_send()

                over(0, count, drain_shift)

            @pl.when(s < sections - 1)
            def _():
                over(0, count, lambda c: af_copy(t, c).wait_send())


def finish_kernel(cfg, gin_ref, gout_ref, h, dyc, res_ref, gin_hbm, gout_hbm, res_hbm, made, sem):
    blocks, ready = cfg
    slots, tokens, local = h.shape
    width = dyc.shape[2]
    span = local // blocks
    step = width // blocks
    copies = []
    for i in range(ready):
        at = pl.ds(i * span, span)
        copies.append(pltpu.make_async_copy(gout_ref.at[0, at], gout_hbm.at[0, at], sem.at[1, i]))
    for i in range(blocks):
        at = pl.ds(i * step, step)
        copies.append(pltpu.make_async_copy(gin_ref.at[0, at], gin_hbm.at[0, at], sem.at[0, i]))
    copies.append(pltpu.make_async_copy(res_ref, res_hbm, sem.at[2, 0]))
    for copy in copies:
        copy.start()
    for i in range(ready, blocks):
        at = pl.ds(i * span, span)
        lhs = jnp.concatenate([h[t, :, at] for t in range(slots)], axis=0)
        made[i - ready] = dot(lhs, dyc[...].reshape(slots * tokens, width), TN).astype(BF16)
        copy = pltpu.make_async_copy(made.at[i - ready], gout_hbm.at[0, at], sem.at[1, i])
        copy.start()
        copies.append(copy)
    for copy in copies:
        copy.wait()


def fast_device(sections, saved_inputs, slot_index, example_lengths, first_grads, loss_grads, w_in, w_out):
    parts = lax.axis_size("tensor")
    slots = loss_grads.shape[0] + 1
    rows, width = first_grads.shape[1:]
    local = w_in.shape[2]
    nz = parts // 2
    tokens = parts * rows
    examples = example_lengths.shape[2]
    chunks = max(1, width // 256)
    sub = 2
    ready = min(1, chunks)
    count = chunks * sub
    part_cols = width // count
    cfg = (sections, parts, nz, slots, rows, width, local, chunks, sub, ready, examples, local * parts)
    hbm = pl.BlockSpec(memory_space=pl.ANY)
    vmem = pl.BlockSpec(memory_space=pltpu.VMEM)
    dma = pltpu.SemaphoreType.DMA
    sds = jax.ShapeDtypeStruct
    flops = 2 * tokens * width * local * slots * 5
    grad_in, grad_out, hidden, scaled, results = pl.pallas_call(
        functools.partial(chain_kernel, cfg),
        out_shape=(
            pltpu.VMEM((1, width, local), BF16),
            pltpu.VMEM((1, local, width), BF16),
            pltpu.VMEM((slots, tokens, local), BF16),
            pltpu.VMEM((slots, tokens, width), BF16),
            pltpu.VMEM((1, slots, rows, width), BF16),
        ),
        in_specs=[pl.BlockSpec(memory_space=pltpu.HBM)] * 7,
        out_specs=[vmem] * 5,
        scratch_shapes=[
            pltpu.VMEM((slots, nz, 2, rows, width), BF16),
            pltpu.VMEM((slots, count, nz, 2, rows, part_cols), BF16),
            pltpu.VMEM((slots, tokens, local), BF16),
            pltpu.VMEM((tokens, local), F32),
            pltpu.VMEM((tokens, local), F32),
            pltpu.VMEM((tokens, tokens), F32),
            pltpu.VMEM((tokens, tokens), F32),
            pltpu.VMEM((count, nz, rows, part_cols), F32),
            pltpu.VMEM((slots, count, nz, rows, part_cols), BF16),
            pltpu.VMEM((slots, count, nz, rows, part_cols), BF16),
            pltpu.VMEM((slots, count, nz, rows, part_cols), BF16),
            pltpu.VMEM((slots, count, nz, rows, part_cols), BF16),
            pltpu.VMEM((slots, count, rows, part_cols), BF16),
            pltpu.VMEM((slots, 8, 128), F32),
            pltpu.VMEM((slots, parts, 8, 128), F32),
            pltpu.VMEM((slots, width, tokens), BF16),
            pltpu.SMEM(slot_index.shape, jnp.int32),
            pltpu.SMEM((1, examples, slots), jnp.int32),
            pltpu.VMEM(saved_inputs.shape[1:], BF16),
            dma((3 + slots * count,)),
            dma((2, 4)),
            dma((2 * slots, nz)), dma((2 * slots, nz)), dma((2 * slots, nz)), dma((2 * slots, nz)),
            dma((slots, count)), dma((slots, count)),
            dma((slots, count, nz)), dma((slots, count, nz)),
            dma((slots - 1, count, nz)), dma((slots - 1, count, nz)),
            dma((slots - 1, count)), dma((slots - 1, count)),
            dma((slots, parts)), dma((slots, parts)),
        ],
        compiler_params=pltpu.CompilerParams(collective_id=0, has_side_effects=True, vmem_limit_bytes=36 * 1024 * 1024),
        cost_estimate=pl.CostEstimate(flops=flops, bytes_accessed=4 * width * local, transcendentals=0),
        name="chain",
    )(slot_index, jnp.swapaxes(example_lengths, 1, 2), saved_inputs, first_grads, loss_grads, w_in, w_out)

    return pl.pallas_call(
        functools.partial(finish_kernel, (chunks, ready)),
        out_shape=(
            sds((1, width, local), BF16),
            sds((1, local, width), BF16),
            sds((1, slots, rows, width), BF16),
        ),
        in_specs=[vmem] * 5,
        out_specs=[hbm] * 3,
        scratch_shapes=[pltpu.VMEM((chunks - ready, local // chunks, width), BF16), dma((3, chunks))],
        compiler_params=pltpu.CompilerParams(vmem_limit_bytes=8 * 1024 * 1024),
        cost_estimate=pl.CostEstimate(flops=2 * slots * tokens * width * local, bytes_accessed=8 * width * local, transcendentals=0),
        name="finish",
    )(grad_in, grad_out, hidden, scaled, results)


def shifted(value, axis, steps):
    count = lax.axis_size(axis)
    first, last = (max(0, -steps), min(count, count - steps))
    return lax.ppermute(value, axis, [(source, source + steps) for source in range(first, last)])


def membership(lengths, tokens):
    ends = jnp.cumsum(lengths)
    position = jnp.arange(tokens, dtype=jnp.int32)
    example_id = jnp.sum((position[:, None] >= ends[None, :-1]).astype(jnp.int32), axis=1)
    labels = jnp.arange(lengths.shape[0], dtype=jnp.int32)
    return (example_id[:, None] == labels[None, :]).astype(F32)


def spread(value, axis):
    copies = jnp.broadcast_to(value[None], (lax.axis_size(axis),) + value.shape)
    return lax.all_to_all(copies, axis, 0, 0)


def gram(value):
    return lax.dot_general(value, value, (((1,), (1,)), ((), ())), preferred_element_type=F32)


def per_device(saved_inputs, slot_index, example_lengths, first_grads, loss_grads, w_in, w_out):
    section_count = lax.axis_size("section")
    parts = lax.axis_size("tensor")
    is_last = lax.axis_index("section") == section_count - 1
    first = w_in[0]
    second = w_out[0]
    slot_count = loss_grads.shape[0] + 1
    rows, width = first_grads.shape[1:]
    hidden_all = first.shape[1] * parts
    picked = [
        lax.dynamic_index_in_dim(saved_inputs[0], slot_index[0, slot], 0, keepdims=False)
        for slot in range(slot_count)
    ]
    tokens = parts * rows
    opening = spread(jnp.concatenate([picked[0], first_grads[0]]), "tensor")
    later = spread(jnp.concatenate(picked[1:]), "tensor")
    every_input = [opening[:, :rows].reshape(tokens, width)]
    for slot in range(slot_count - 1):
        every_input.append(later[:, slot * rows : (slot + 1) * rows].reshape(tokens, width))
    incoming = first_grads[0]
    results, dzs, hiddens, grad_list, members, squares = [], [], [], [], [], []
    for slot in range(slot_count):
        inputs = every_input[slot]
        if slot == 0:
            grads = opening[:, rows:].reshape(tokens, width)
        else:
            grads = spread(incoming, "tensor").reshape(tokens, width)
        z = jnp.dot(inputs, first, preferred_element_type=F32)
        relu = jnp.maximum(z, 0.0)
        hidden = (relu * relu).astype(BF16)
        back = jnp.einsum("td,fd->tf", grads, second, preferred_element_type=F32)
        dz = (2.0 * relu * back).astype(BF16)
        own_terms = jnp.einsum("tf,df->td", dz, first, preferred_element_type=F32).astype(BF16)
        pieces = lax.all_to_all(own_terms.reshape(parts, rows, width), "tensor", 0, 0)
        shares = jnp.sum(pieces.astype(F32), axis=0)
        passing = (incoming.astype(F32) + shares).astype(BF16)
        results.append(passing)
        if slot + 1 < slot_count:
            arrived = shifted(passing, "section", -1)
            incoming = jnp.where(is_last, loss_grads[slot], arrived)
        member = membership(example_lengths[0, slot], inputs.shape[0])
        paired = gram(inputs) * gram(dz) + gram(hidden) * gram(grads)
        per_row = jnp.stack([jnp.sum(paired * member[:, e][None, :], axis=1) for e in range(member.shape[1])], axis=1)
        squares.append(jnp.sum(member * per_row, axis=0))
        dzs.append(dz)
        hiddens.append(hidden)
        grad_list.append(grads)
        members.append(member)
    local = jnp.stack(squares)
    total = jnp.sum(spread(local, "tensor"), axis=0)
    factor = 1.0 / (jnp.sqrt(total / (width * hidden_all)) + GAMMA)
    token_factor = jnp.concatenate([jnp.sum(m * factor[i][None, :], axis=1) for i, m in enumerate(members)])[:, None]
    xc = (jnp.concatenate(every_input).astype(F32) * token_factor).astype(BF16)
    dyc = (jnp.concatenate(grad_list).astype(F32) * token_factor).astype(BF16)
    grad_in = jnp.einsum("td,tf->df", xc, jnp.concatenate(dzs), preferred_element_type=F32).astype(BF16)[None]
    grad_out = jnp.einsum("tf,td->fd", jnp.concatenate(hiddens), dyc, preferred_element_type=F32).astype(BF16)[None]
    input_grads = jnp.stack(results)[None]
    return (grad_in, grad_out, input_grads)


def solution(mesh):
    sections = mesh.shape["section"]
    parts = mesh.shape["tensor"]

    def body(saved_inputs, slot_index, example_lengths, first_grads, loss_grads, w_in, w_out):
        rows, width = first_grads.shape[1:]
        fits = sections > 2 and parts % 2 == 0 and rows % 16 == 0 and width % 256 == 0 and w_in.shape[2] % 512 == 0 and loss_grads.shape[0] > 0
        run = functools.partial(fast_device, sections) if fits else per_device
        return run(saved_inputs, slot_index, example_lengths, first_grads, loss_grads, w_in, w_out)

    return jax.shard_map(
        body,
        mesh=mesh,
        in_specs=(
            P("section", None, "tensor", None),
            P("section", None),
            P("section", None, None),
            P("section", "tensor", None),
            P(None, "tensor", None),
            P("section", None, "tensor"),
            P("section", "tensor", None),
        ),
        out_specs=(
            P("section", None, "tensor"),
            P("section", "tensor", None),
            P("section", None, "tensor", None),
        ),
        check_vma=False,
    )
```

```python
import functools

import jax
import jax.numpy as jnp
from jax import lax
from jax.experimental import pallas as pl
from jax.experimental.pallas import tpu as pltpu
from jax.sharding import PartitionSpec as P

GAMMA = 0.01
F32 = jnp.float32
BF16 = jnp.bfloat16
MESH = pl.DeviceIdType.MESH
NT = (((1,), (1,)), ((), ()))
TN = (((0,), (0,)), ((), ()))


def dot(a, b, dims):
    return lax.dot_general(a, b, dims, preferred_element_type=F32)


def chain_kernel(
    cfg,
    index_hbm, lengths_hbm, saved_hbm, first_hbm, loss_hbm, win_hbm, wout_hbm,
    gin_ref, gout_ref, h, dyc, res_ref,
    xg, dyb, dz, rbuf, acc, gxs, ghs, own, rxs, rxr, rzs, rzr, res, sqs, sqr, xct,
    index_ref, lengths_ref, saved_ref, in_sem,
    w_sem, ag_send, ag_recv, fw_send, fw_recv, rx_send, rx_recv, rz_send, rz_recv,
    sh_send, sh_recv, af_send, af_recv, sq_send, sq_recv,
):
    sections, parts, nz, slots, rows, width, local, chunks, sub, ready, examples, hidden_all = cfg
    cols = width // chunks
    count = chunks * sub
    part_cols = cols // sub
    tokens = parts * rows
    win, wout = gin_ref.at[0], gout_ref.at[0]
    span = local // chunks
    s = lax.axis_index("section")
    p = lax.axis_index("tensor")
    z = p // 2
    x = p % 2
    is_last = s == sections - 1
    partner = {"section": s, "tensor": z * 2 + (1 - x)}

    def zpeer(j):
        return {"section": s, "tensor": ((z + j) % nz) * 2 + x}

    def behind(j):
        return {"section": s - 1, "tensor": ((z + j) % nz) * 2 + x}

    index_in = pltpu.make_async_copy(index_hbm, index_ref, in_sem.at[0])
    lengths_in = pltpu.make_async_copy(lengths_hbm, lengths_ref, in_sem.at[1])
    saved_in = pltpu.make_async_copy(saved_hbm.at[0], saved_ref, in_sem.at[2])
    index_in.start()
    saved_in.start()
    lengths_in.start()

    def grads_in(t, c):
        source = first_hbm.at[0] if t == 0 else loss_hbm.at[t - 1]
        return pltpu.make_async_copy(source.at[:, c * part_cols:(c + 1) * part_cols], dyb.at[t, c, z, x], in_sem.at[3 + t * count + c])

    for c in range(count):
        grads_in(0, c).start()

    @pl.when(is_last)
    def _():
        for t in range(1, slots):
            for c in range(count):
                grads_in(t, c).start()

    pieces = 4
    span_in, span_out = local // pieces, local // pieces
    for k in range(pieces):
        pltpu.make_async_copy(win_hbm.at[0, :, pl.ds(k * span_in, span_in)], win.at[:, pl.ds(k * span_in, span_in)], w_sem.at[0, k]).start()
    for k in range(pieces):
        pltpu.make_async_copy(wout_hbm.at[0, pl.ds(k * span_out, span_out)], wout.at[pl.ds(k * span_out, span_out)], w_sem.at[1, k]).start()

    barrier = pltpu.get_barrier_semaphore()
    for j in range(1, parts):
        pl.semaphore_signal(barrier, inc=1, device_id={"section": s, "tensor": (p + j) % parts}, device_id_type=MESH)

    for side in (1, sections - 1):
        for j in range(nz):
            pl.semaphore_signal(barrier, inc=1, device_id={"section": (s + side) % sections, "tensor": ((z + j) % nz) * 2 + x}, device_id_type=MESH)
    index_in.wait()
    saved_in.wait()
    for t in range(slots):
        xg[t, z, x] = saved_ref[index_ref[0, t]]
    for c in range(count):
        grads_in(0, c).wait()
    lengths_in.wait()

    @pl.when(is_last)
    def _():
        for t in range(1, slots):
            for c in range(count):
                grads_in(t, c).wait()

    pl.semaphore_wait(barrier, parts - 1 + 2 * nz)

    def block(k, source):
        if k < slots:
            return xg.at[k, source, x]
        return dyb.at[k - slots, :, source, x]

    def ag_copy(k, j, to_partner):
        if to_partner:
            ref = block(k, (z + nz - j) % nz)
            return pltpu.make_async_remote_copy(ref, ref, fw_send.at[k, j], fw_recv.at[k, j], device_id=partner, device_id_type=MESH)
        ref = block(k, z)
        return pltpu.make_async_remote_copy(ref, ref, ag_send.at[k, j], ag_recv.at[k, j], device_id=zpeer(j), device_id_type=MESH)

    def ag_open(k):
        for j in range(1, nz):
            ag_copy(k, j, False).start()

    def ag_forward(k):
        ag_copy(k, 0, True).start()
        for j in range(1, nz):
            ag_copy(k, j, False).wait_recv()
            ag_copy(k, j, True).start()

    def ag_finish(k):
        for j in range(nz):
            ag_copy(k, j, True).wait_recv()

    def ag_drain(k):
        for j in range(nz):
            if j:
                ag_copy(k, j, False).wait_send()
            ag_copy(k, j, True).wait_send()

    def grads_of(t, lo, hi):
        return jnp.concatenate([dyb[t, c].reshape(tokens, part_cols) for c in range(lo, hi)], axis=1)

    def z_tile(t, i, size):
        at = pl.ds(pl.multiple_of(i * size, size), size)
        zz = jnp.dot(xg[t].reshape(tokens, width), win[:, at], preferred_element_type=F32)
        r = jnp.maximum(zz, 0.0)
        rbuf[:, at] = r
        h[t, :, at] = (r * r).astype(BF16)

    def back_tile(t, i, size):
        at = pl.ds(pl.multiple_of(i * size, size), size)
        dh = dot(grads_of(t, 0, count), wout[at, :], NT)
        dz[t, :, at] = (2.0 * rbuf[:, at] * dh).astype(BF16)

    def back_chunk(t, c, mode):
        size = min(2048, local)

        def body(i, carry):
            at = pl.ds(pl.multiple_of(i * size, size), size)
            dh = dot(grads_of(t, c * sub, (c + 1) * sub), wout[at, c * cols:(c + 1) * cols], NT)
            if mode > 0:
                dh = dh + acc[:, at]
            if mode < 2:
                acc[:, at] = dh
            else:
                dz[t, :, at] = (2.0 * rbuf[:, at] * dh).astype(BF16)
            return carry

        lax.fori_loop(0, local // size, body, 0)

    def rx_copy(t, c):
        return pltpu.make_async_remote_copy(rxs.at[t, c], rxr.at[t, c], rx_send.at[t, c], rx_recv.at[t, c], device_id=partner, device_id_type=MESH)

    def rz_copy(t, c, j):
        return pltpu.make_async_remote_copy(rzs.at[t, c, (z + j) % nz], rzr.at[t, c, j], rz_send.at[t, c, j], rz_recv.at[t, c, j], device_id=zpeer(j), device_id_type=MESH)

    def sh_copy(t, c, j):
        return pltpu.make_async_remote_copy(res.at[t, c], dyb.at[t + 1, c, z, x], sh_send.at[t, c, j], sh_recv.at[t, c, j], device_id=behind(j), device_id_type=MESH)

    def af_copy(t, c):
        ref = dyb.at[t + 1, c, :, x]
        return pltpu.make_async_remote_copy(ref, ref, af_send.at[t, c], af_recv.at[t, c], device_id=partner, device_id_type=MESH)

    def over(lo, hi, body):
        def step(c, carry):
            body(c)
            return carry

        lax.fori_loop(lo, hi, step, 0)

    def partial_dx(t):
        def body(c):
            wide = win[pl.ds(pl.multiple_of(c * cols, cols), cols), :]
            whole = dot(dz[t], wide, NT)
            for u in range(sub):
                part = whole[:, u * part_cols:(u + 1) * part_cols].reshape(nz, 2, rows, part_cols)
                first_half, second_half = part[:, 0], part[:, 1]
                mine = jnp.where(x == 0, first_half, second_half)
                other = jnp.where(x == 0, second_half, first_half)
                own[c * sub + u] = mine
                rxs[t, c * sub + u] = other.astype(BF16)
                rx_copy(t, c * sub + u).start()

        over(0, chunks, body)

    def pair_sum(t, c):
        rx_copy(t, c).wait_recv()
        total = own[c] + rxr[t, c].astype(F32)
        own[c] = total
        rzs[t, c] = total.astype(BF16)
        for j in range(1, nz):
            rz_copy(t, c, j).start()

    def line_sum(t, c):
        total = own[c, z] + dyb[t, c, z, x].astype(F32)
        for j in range(1, nz):
            rz_copy(t, c, j).wait_recv()
            total = total + rzr[t, c, j].astype(F32)
        res[t, c] = total.astype(BF16)
        if t + 1 < slots:
            @pl.when(s > 0)
            def _():
                for j in range(nz):
                    sh_copy(t, c, j).start()

    def hand_over(t, c):
        for j in range(nz):
            sh_copy(t, c, j).wait_recv()
        af_copy(t, c).start()

    def example_mask(t):
        position = lax.broadcasted_iota(jnp.int32, (tokens, 1), 0)
        across = lax.broadcasted_iota(jnp.int32, (1, tokens), 1)
        down, along = [], []
        start = jnp.int32(0)
        for e in range(examples):
            stop = start + lengths_ref[0, e, t]
            if e == examples - 1:
                stop = jnp.int32(tokens)
            down.append((position >= start) & (position < stop))
            along.append((across >= start) & (across < stop))
            start = stop
        return down, along

    def sq_copy(t, j):
        return pltpu.make_async_remote_copy(sqs.at[t], sqr.at[t, j], sq_send.at[t, j], sq_recv.at[t, j], device_id={"section": s, "tensor": (p + j) % parts}, device_id_type=MESH)

    def grams(t):
        inputs = xg[t].reshape(tokens, width)
        gxs[...] = dot(inputs, inputs, NT)
        ghs[...] = dot(h[t], h[t], NT)

    def squares(t):
        grads = grads_of(t, 0, count)
        paired = gxs[...] * dot(dz[t], dz[t], NT) + ghs[...] * dot(grads, grads, NT)
        down, along = example_mask(t)
        row = lax.broadcasted_iota(jnp.int32, (8, 128), 0)
        out = jnp.zeros((8, 128), F32)
        for e in range(examples):
            kept = jnp.where(down[e], paired, 0.0)
            kept = jnp.where(along[e], kept, 0.0)
            value = jnp.sum(jnp.sum(kept, axis=0, keepdims=True), axis=1, keepdims=True)
            out = jnp.where(row == e, value, out)
        sqs[t] = out
        for j in range(1, parts):
            sq_copy(t, j).start()

    def factors(t):
        total = sqs[t]
        for j in range(1, parts):
            sq_copy(t, j).wait_recv()
            total = total + sqr[t, j]
        factor = 1.0 / (jnp.sqrt(total / (width * hidden_all)) + GAMMA)
        down, _ = example_mask(t)
        per_token = jnp.zeros((tokens, 1), F32)
        for e in range(examples):
            per_token = jnp.where(down[e], factor[e:e + 1, 0:1], per_token)
        return per_token

    def scale(t, k, per_token):
        at = slice(k * part_cols, (k + 1) * part_cols)
        scaled = xg[t, :, :, :, at].reshape(tokens, part_cols).astype(F32) * per_token
        xct[t, at] = scaled.T.astype(BF16)
        dyc[t, :, at] = (dyb[t, k].reshape(tokens, part_cols).astype(F32) * per_token).astype(BF16)

    def grad_in_block(i):
        at = pl.ds(i * span, span)
        lhs = jnp.concatenate([xct[t] for t in range(slots)], axis=1)
        rhs = jnp.concatenate([dz[t, :, at] for t in range(slots)], axis=0)
        win[:, at] = jnp.dot(lhs, rhs, preferred_element_type=F32).astype(BF16)

    def grad_out_block(i):
        at = pl.ds(i * span, span)
        lhs = jnp.concatenate([h[t, :, at] for t in range(slots)], axis=0)
        wout[at, :] = dot(lhs, dyc[...].reshape(slots * tokens, width), TN).astype(BF16)

    end = slots - 1
    ag_open(0)
    ag_open(slots)
    if end > 0:
        ag_open(1)

        @pl.when(is_last)
        def _():
            ag_open(slots + 1)

    ag_forward(0)
    ag_forward(slots)
    for k in range(pieces):
        pltpu.make_async_copy(win_hbm.at[0, :, pl.ds(k * span_in, span_in)], win.at[:, pl.ds(k * span_in, span_in)], w_sem.at[0, k]).wait()
    ag_finish(0)
    over(0, 2, lambda i: z_tile(0, i, local // 2))
    grams(0)
    for k in range(pieces):
        pltpu.make_async_copy(wout_hbm.at[0, pl.ds(k * span_out, span_out)], wout.at[pl.ds(k * span_out, span_out)], w_sem.at[1, k]).wait()
    ag_finish(slots)
    over(0, 2, lambda i: back_tile(0, i, local // 2))

    for t in range(end):
        partial_dx(t)
        ag_forward(t + 1)
        if t > 0:
            grams(t)
        squares(t)
        over(0, count, lambda k: pair_sum(t, k))

        @pl.when(is_last)
        def _():
            ag_forward(slots + t + 1)

        per_token = None
        for k in range(count):
            line_sum(t, k)
            if k == 1:
                per_token = factors(t)
            if k > 1:
                scale(t, k - 2, per_token)
        if t + 2 < slots:
            ag_open(t + 2)

            @pl.when(is_last)
            def _():
                ag_open(slots + t + 2)

        for k in range(count - 2, count):
            scale(t, k, per_token)
        ag_finish(t + 1)

        def tile_and_hand(c):
            @pl.when(s < sections - 1)
            def _():
                for u in range(sub):
                    hand_over(t, c * sub + u)

            z_tile(t + 1, c, span)

        over(0, chunks, tile_and_hand)
        if t + 1 == end:
            grams(end)

        @pl.when(is_last)
        def _():
            ag_finish(slots + t + 1)

        for c in range(chunks):
            @pl.when(s < sections - 1)
            def _():
                for u in range(sub):
                    af_copy(t, c * sub + u).wait_recv()

            back_chunk(t + 1, c, 0 if c == 0 else (2 if c == chunks - 1 else 1))

    squares(end)
    partial_dx(end)
    per_token = factors(end)
    for k in range(count):
        scale(end, k, per_token)
    for c in range(chunks):
        for k in range(count):
            if min(chunks - 1, (k + 2) // 3) == c:
                pair_sum(end, k)
        grad_in_block(c)
    for i in range(ready):
        grad_out_block(i)
    over(0, count, lambda k: line_sum(end, k))

    for t in range(slots):
        for c in range(count):
            res_ref[0, t, :, c * part_cols:(c + 1) * part_cols] = res[t, c]

    for t in range(slots):
        ag_drain(t)
    ag_drain(slots)

    @pl.when(is_last)
    def _():
        for t in range(1, slots):
            ag_drain(slots + t)

    for t in range(slots):
        def drain(c):
            rx_copy(t, c).wait_send()
            for j in range(1, nz):
                rz_copy(t, c, j).wait_send()

        over(0, count, drain)
        for j in range(1, parts):
            sq_copy(t, j).wait_send()
        if t + 1 < slots:
            @pl.when(s > 0)
            def _():
                def drain_shift(c):
                    for j in range(nz):
                        sh_copy(t, c, j).wait_send()

                over(0, count, drain_shift)

            @pl.when(s < sections - 1)
            def _():
                over(0, count, lambda c: af_copy(t, c).wait_send())


def finish_kernel(cfg, gin_ref, gout_ref, h, dyc, res_ref, gin_hbm, gout_hbm, res_hbm, made, sem):
    blocks, ready = cfg
    slots, tokens, local = h.shape
    width = dyc.shape[2]
    span = local // blocks
    step = width // blocks
    copies = []
    for i in range(ready):
        at = pl.ds(i * span, span)
        copies.append(pltpu.make_async_copy(gout_ref.at[0, at], gout_hbm.at[0, at], sem.at[1, i]))
    for i in range(blocks):
        at = pl.ds(i * step, step)
        copies.append(pltpu.make_async_copy(gin_ref.at[0, at], gin_hbm.at[0, at], sem.at[0, i]))
    copies.append(pltpu.make_async_copy(res_ref, res_hbm, sem.at[2, 0]))
    for copy in copies:
        copy.start()
    for i in range(ready, blocks):
        at = pl.ds(i * span, span)
        lhs = jnp.concatenate([h[t, :, at] for t in range(slots)], axis=0)
        made[i - ready] = dot(lhs, dyc[...].reshape(slots * tokens, width), TN).astype(BF16)
        copy = pltpu.make_async_copy(made.at[i - ready], gout_hbm.at[0, at], sem.at[1, i])
        copy.start()
        copies.append(copy)
    for copy in copies:
        copy.wait()


def fast_device(sections, saved_inputs, slot_index, example_lengths, first_grads, loss_grads, w_in, w_out):
    parts = lax.axis_size("tensor")
    slots = loss_grads.shape[0] + 1
    rows, width = first_grads.shape[1:]
    local = w_in.shape[2]
    nz = parts // 2
    tokens = parts * rows
    examples = example_lengths.shape[2]
    chunks = max(1, width // 256)
    sub = 1
    ready = min(1, chunks)
    count = chunks * sub
    part_cols = width // count
    cfg = (sections, parts, nz, slots, rows, width, local, chunks, sub, ready, examples, local * parts)
    hbm = pl.BlockSpec(memory_space=pl.ANY)
    vmem = pl.BlockSpec(memory_space=pltpu.VMEM)
    dma = pltpu.SemaphoreType.DMA
    sds = jax.ShapeDtypeStruct
    flops = 2 * tokens * width * local * slots * 5
    grad_in, grad_out, hidden, scaled, results = pl.pallas_call(
        functools.partial(chain_kernel, cfg),
        out_shape=(
            pltpu.VMEM((1, width, local), BF16),
            pltpu.VMEM((1, local, width), BF16),
            pltpu.VMEM((slots, tokens, local), BF16),
            pltpu.VMEM((slots, tokens, width), BF16),
            pltpu.VMEM((1, slots, rows, width), BF16),
        ),
        in_specs=[pl.BlockSpec(memory_space=pltpu.HBM)] * 7,
        out_specs=[vmem] * 5,
        scratch_shapes=[
            pltpu.VMEM((slots, nz, 2, rows, width), BF16),
            pltpu.VMEM((slots, count, nz, 2, rows, part_cols), BF16),
            pltpu.VMEM((slots, tokens, local), BF16),
            pltpu.VMEM((tokens, local), F32),
            pltpu.VMEM((tokens, local), F32),
            pltpu.VMEM((tokens, tokens), F32),
            pltpu.VMEM((tokens, tokens), F32),
            pltpu.VMEM((count, nz, rows, part_cols), F32),
            pltpu.VMEM((slots, count, nz, rows, part_cols), BF16),
            pltpu.VMEM((slots, count, nz, rows, part_cols), BF16),
            pltpu.VMEM((slots, count, nz, rows, part_cols), BF16),
            pltpu.VMEM((slots, count, nz, rows, part_cols), BF16),
            pltpu.VMEM((slots, count, rows, part_cols), BF16),
            pltpu.VMEM((slots, 8, 128), F32),
            pltpu.VMEM((slots, parts, 8, 128), F32),
            pltpu.VMEM((slots, width, tokens), BF16),
            pltpu.SMEM(slot_index.shape, jnp.int32),
            pltpu.SMEM((1, examples, slots), jnp.int32),
            pltpu.VMEM(saved_inputs.shape[1:], BF16),
            dma((3 + slots * count,)),
            dma((2, 4)),
            dma((2 * slots, nz)), dma((2 * slots, nz)), dma((2 * slots, nz)), dma((2 * slots, nz)),
            dma((slots, count)), dma((slots, count)),
            dma((slots, count, nz)), dma((slots, count, nz)),
            dma((slots - 1, count, nz)), dma((slots - 1, count, nz)),
            dma((slots - 1, count)), dma((slots - 1, count)),
            dma((slots, parts)), dma((slots, parts)),
        ],
        compiler_params=pltpu.CompilerParams(collective_id=0, has_side_effects=True, vmem_limit_bytes=36 * 1024 * 1024),
        cost_estimate=pl.CostEstimate(flops=flops, bytes_accessed=4 * width * local, transcendentals=0),
        name="chain",
    )(slot_index, jnp.swapaxes(example_lengths, 1, 2), saved_inputs, first_grads, loss_grads, w_in, w_out)

    return pl.pallas_call(
        functools.partial(finish_kernel, (chunks, ready)),
        out_shape=(
            sds((1, width, local), BF16),
            sds((1, local, width), BF16),
            sds((1, slots, rows, width), BF16),
        ),
        in_specs=[vmem] * 5,
        out_specs=[hbm] * 3,
        scratch_shapes=[pltpu.VMEM((chunks - ready, local // chunks, width), BF16), dma((3, chunks))],
        compiler_params=pltpu.CompilerParams(vmem_limit_bytes=8 * 1024 * 1024),
        cost_estimate=pl.CostEstimate(flops=2 * slots * tokens * width * local, bytes_accessed=8 * width * local, transcendentals=0),
        name="finish",
    )(grad_in, grad_out, hidden, scaled, results)


def shifted(value, axis, steps):
    count = lax.axis_size(axis)
    first, last = (max(0, -steps), min(count, count - steps))
    return lax.ppermute(value, axis, [(source, source + steps) for source in range(first, last)])


def membership(lengths, tokens):
    ends = jnp.cumsum(lengths)
    position = jnp.arange(tokens, dtype=jnp.int32)
    example_id = jnp.sum((position[:, None] >= ends[None, :-1]).astype(jnp.int32), axis=1)
    labels = jnp.arange(lengths.shape[0], dtype=jnp.int32)
    return (example_id[:, None] == labels[None, :]).astype(F32)


def spread(value, axis):
    copies = jnp.broadcast_to(value[None], (lax.axis_size(axis),) + value.shape)
    return lax.all_to_all(copies, axis, 0, 0)


def gram(value):
    return lax.dot_general(value, value, (((1,), (1,)), ((), ())), preferred_element_type=F32)


def per_device(saved_inputs, slot_index, example_lengths, first_grads, loss_grads, w_in, w_out):
    section_count = lax.axis_size("section")
    parts = lax.axis_size("tensor")
    is_last = lax.axis_index("section") == section_count - 1
    first = w_in[0]
    second = w_out[0]
    slot_count = loss_grads.shape[0] + 1
    rows, width = first_grads.shape[1:]
    hidden_all = first.shape[1] * parts
    picked = [
        lax.dynamic_index_in_dim(saved_inputs[0], slot_index[0, slot], 0, keepdims=False)
        for slot in range(slot_count)
    ]
    tokens = parts * rows
    opening = spread(jnp.concatenate([picked[0], first_grads[0]]), "tensor")
    later = spread(jnp.concatenate(picked[1:]), "tensor")
    every_input = [opening[:, :rows].reshape(tokens, width)]
    for slot in range(slot_count - 1):
        every_input.append(later[:, slot * rows : (slot + 1) * rows].reshape(tokens, width))
    incoming = first_grads[0]
    results, dzs, hiddens, grad_list, members, squares = [], [], [], [], [], []
    for slot in range(slot_count):
        inputs = every_input[slot]
        if slot == 0:
            grads = opening[:, rows:].reshape(tokens, width)
        else:
            grads = spread(incoming, "tensor").reshape(tokens, width)
        z = jnp.dot(inputs, first, preferred_element_type=F32)
        relu = jnp.maximum(z, 0.0)
        hidden = (relu * relu).astype(BF16)
        back = jnp.einsum("td,fd->tf", grads, second, preferred_element_type=F32)
        dz = (2.0 * relu * back).astype(BF16)
        own_terms = jnp.einsum("tf,df->td", dz, first, preferred_element_type=F32).astype(BF16)
        pieces = lax.all_to_all(own_terms.reshape(parts, rows, width), "tensor", 0, 0)
        shares = jnp.sum(pieces.astype(F32), axis=0)
        passing = (incoming.astype(F32) + shares).astype(BF16)
        results.append(passing)
        if slot + 1 < slot_count:
            arrived = shifted(passing, "section", -1)
            incoming = jnp.where(is_last, loss_grads[slot], arrived)
        member = membership(example_lengths[0, slot], inputs.shape[0])
        paired = gram(inputs) * gram(dz) + gram(hidden) * gram(grads)
        per_row = jnp.stack([jnp.sum(paired * member[:, e][None, :], axis=1) for e in range(member.shape[1])], axis=1)
        squares.append(jnp.sum(member * per_row, axis=0))
        dzs.append(dz)
        hiddens.append(hidden)
        grad_list.append(grads)
        members.append(member)
    local = jnp.stack(squares)
    total = jnp.sum(spread(local, "tensor"), axis=0)
    factor = 1.0 / (jnp.sqrt(total / (width * hidden_all)) + GAMMA)
    token_factor = jnp.concatenate([jnp.sum(m * factor[i][None, :], axis=1) for i, m in enumerate(members)])[:, None]
    xc = (jnp.concatenate(every_input).astype(F32) * token_factor).astype(BF16)
    dyc = (jnp.concatenate(grad_list).astype(F32) * token_factor).astype(BF16)
    grad_in = jnp.einsum("td,tf->df", xc, jnp.concatenate(dzs), preferred_element_type=F32).astype(BF16)[None]
    grad_out = jnp.einsum("tf,td->fd", jnp.concatenate(hiddens), dyc, preferred_element_type=F32).astype(BF16)[None]
    input_grads = jnp.stack(results)[None]
    return (grad_in, grad_out, input_grads)


def solution(mesh):
    sections = mesh.shape["section"]
    parts = mesh.shape["tensor"]

    def body(saved_inputs, slot_index, example_lengths, first_grads, loss_grads, w_in, w_out):
        rows, width = first_grads.shape[1:]
        fits = sections > 2 and parts % 2 == 0 and rows % 16 == 0 and width % 256 == 0 and w_in.shape[2] % 512 == 0 and loss_grads.shape[0] > 0
        run = functools.partial(fast_device, sections) if fits else per_device
        return run(saved_inputs, slot_index, example_lengths, first_grads, loss_grads, w_in, w_out)

    return jax.shard_map(
        body,
        mesh=mesh,
        in_specs=(
            P("section", None, "tensor", None),
            P("section", None),
            P("section", None, None),
            P("section", "tensor", None),
            P(None, "tensor", None),
            P("section", None, "tensor"),
            P("section", "tensor", None),
        ),
        out_specs=(
            P("section", None, "tensor"),
            P("section", "tensor", None),
            P("section", None, "tensor", None),
        ),
        check_vma=False,
    )
```

```python
import functools

import jax
import jax.numpy as jnp
from jax import lax
from jax.experimental import pallas as pl
from jax.experimental.pallas import tpu as pltpu
from jax.sharding import PartitionSpec as P

GAMMA = 0.01
F32 = jnp.float32
BF16 = jnp.bfloat16
MESH = pl.DeviceIdType.MESH
NT = (((1,), (1,)), ((), ()))
TN = (((0,), (0,)), ((), ()))


def dot(a, b, dims):
    return lax.dot_general(a, b, dims, preferred_element_type=F32)


def chain_kernel(
    cfg,
    index_hbm, lengths_hbm, saved_hbm, first_hbm, loss_hbm, win_hbm, wout_hbm,
    gin_ref, gout_ref, h, dyc, res_ref,
    xg, dyb, dz, rbuf, acc, gxs, ghs, own, rxs, rxr, rzs, rzr, res, sqs, sqr, xct,
    index_ref, lengths_ref, saved_ref, in_sem,
    w_sem, ag_send, ag_recv, fw_send, fw_recv, rx_send, rx_recv, rz_send, rz_recv,
    sh_send, sh_recv, af_send, af_recv, sq_send, sq_recv,
):
    sections, parts, nz, slots, rows, width, local, chunks, sub, ready, examples, hidden_all = cfg
    cols = width // chunks
    count = chunks * sub
    part_cols = cols // sub
    tokens = parts * rows
    win, wout = gin_ref.at[0], gout_ref.at[0]
    span = local // chunks
    s = lax.axis_index("section")
    p = lax.axis_index("tensor")
    z = p // 2
    x = p % 2
    is_last = s == sections - 1
    partner = {"section": s, "tensor": z * 2 + (1 - x)}

    def zpeer(j):
        return {"section": s, "tensor": ((z + j) % nz) * 2 + x}

    def behind(j):
        return {"section": s - 1, "tensor": ((z + j) % nz) * 2 + x}

    index_in = pltpu.make_async_copy(index_hbm, index_ref, in_sem.at[0])
    lengths_in = pltpu.make_async_copy(lengths_hbm, lengths_ref, in_sem.at[1])
    saved_in = pltpu.make_async_copy(saved_hbm.at[0], saved_ref, in_sem.at[2])
    index_in.start()
    saved_in.start()
    lengths_in.start()

    def grads_in(t, c):
        source = first_hbm.at[0] if t == 0 else loss_hbm.at[t - 1]
        return pltpu.make_async_copy(source.at[:, c * part_cols:(c + 1) * part_cols], dyb.at[t, c, z, x], in_sem.at[3 + t * count + c])

    for c in range(count):
        grads_in(0, c).start()

    @pl.when(is_last)
    def _():
        for t in range(1, slots):
            for c in range(count):
                grads_in(t, c).start()

    pieces = 4
    span_in, span_out = local // pieces, local // pieces
    for k in range(pieces):
        pltpu.make_async_copy(win_hbm.at[0, :, pl.ds(k * span_in, span_in)], win.at[:, pl.ds(k * span_in, span_in)], w_sem.at[0, k]).start()
    for k in range(pieces):
        pltpu.make_async_copy(wout_hbm.at[0, pl.ds(k * span_out, span_out)], wout.at[pl.ds(k * span_out, span_out)], w_sem.at[1, k]).start()

    barrier = pltpu.get_barrier_semaphore()
    for j in range(1, parts):
        pl.semaphore_signal(barrier, inc=1, device_id={"section": s, "tensor": (p + j) % parts}, device_id_type=MESH)

    for side in (1, sections - 1):
        for j in range(nz):
            pl.semaphore_signal(barrier, inc=1, device_id={"section": (s + side) % sections, "tensor": ((z + j) % nz) * 2 + x}, device_id_type=MESH)
    index_in.wait()
    saved_in.wait()
    for t in range(slots):
        xg[t, z, x] = saved_ref[index_ref[0, t]]
    for c in range(count):
        grads_in(0, c).wait()
    lengths_in.wait()

    @pl.when(is_last)
    def _():
        for t in range(1, slots):
            for c in range(count):
                grads_in(t, c).wait()

    pl.semaphore_wait(barrier, parts - 1 + 2 * nz)

    def block(k, source):
        if k < slots:
            return xg.at[k, source, x]
        return dyb.at[k - slots, :, source, x]

    def ag_copy(k, j, to_partner):
        if to_partner:
            ref = block(k, (z + nz - j) % nz)
            return pltpu.make_async_remote_copy(ref, ref, fw_send.at[k, j], fw_recv.at[k, j], device_id=partner, device_id_type=MESH)
        ref = block(k, z)
        return pltpu.make_async_remote_copy(ref, ref, ag_send.at[k, j], ag_recv.at[k, j], device_id=zpeer(j), device_id_type=MESH)

    def ag_open(k):
        for j in range(1, nz):
            ag_copy(k, j, False).start()

    def ag_forward(k):
        ag_copy(k, 0, True).start()
        for j in range(1, nz):
            ag_copy(k, j, False).wait_recv()
            ag_copy(k, j, True).start()

    def ag_finish(k):
        for j in range(nz):
            ag_copy(k, j, True).wait_recv()

    def ag_drain(k):
        for j in range(nz):
            if j:
                ag_copy(k, j, False).wait_send()
            ag_copy(k, j, True).wait_send()

    def grads_of(t, lo, hi):
        return jnp.concatenate([dyb[t, c].reshape(tokens, part_cols) for c in range(lo, hi)], axis=1)

    def z_tile(t, i, size):
        at = pl.ds(pl.multiple_of(i * size, size), size)
        zz = jnp.dot(xg[t].reshape(tokens, width), win[:, at], preferred_element_type=F32)
        r = jnp.maximum(zz, 0.0)
        rbuf[:, at] = r
        h[t, :, at] = (r * r).astype(BF16)

    def back_tile(t, i, size):
        at = pl.ds(pl.multiple_of(i * size, size), size)
        dh = dot(grads_of(t, 0, count), wout[at, :], NT)
        dz[t, :, at] = (2.0 * rbuf[:, at] * dh).astype(BF16)

    def back_chunk(t, c, mode):
        size = min(2048, local)

        def body(i, carry):
            at = pl.ds(pl.multiple_of(i * size, size), size)
            dh = dot(grads_of(t, c * sub, (c + 1) * sub), wout[at, c * cols:(c + 1) * cols], NT)
            if mode > 0:
                dh = dh + acc[:, at]
            if mode < 2:
                acc[:, at] = dh
            else:
                dz[t, :, at] = (2.0 * rbuf[:, at] * dh).astype(BF16)
            return carry

        lax.fori_loop(0, local // size, body, 0)

    def rx_copy(t, c):
        return pltpu.make_async_remote_copy(rxs.at[t, c], rxr.at[t, c], rx_send.at[t, c], rx_recv.at[t, c], device_id=partner, device_id_type=MESH)

    def rz_copy(t, c, j):
        return pltpu.make_async_remote_copy(rzs.at[t, c, (z + j) % nz], rzr.at[t, c, j], rz_send.at[t, c, j], rz_recv.at[t, c, j], device_id=zpeer(j), device_id_type=MESH)

    def sh_copy(t, c, j):
        return pltpu.make_async_remote_copy(res.at[t, c], dyb.at[t + 1, c, z, x], sh_send.at[t, c, j], sh_recv.at[t, c, j], device_id=behind(j), device_id_type=MESH)

    def af_copy(t, c):
        ref = dyb.at[t + 1, c, :, x]
        return pltpu.make_async_remote_copy(ref, ref, af_send.at[t, c], af_recv.at[t, c], device_id=partner, device_id_type=MESH)

    def over(lo, hi, body):
        def step(c, carry):
            body(c)
            return carry

        lax.fori_loop(lo, hi, step, 0)

    def partial_dx(t):
        def body(c):
            wide = win[pl.ds(pl.multiple_of(c * cols, cols), cols), :]
            whole = dot(dz[t], wide, NT)
            for u in range(sub):
                part = whole[:, u * part_cols:(u + 1) * part_cols].reshape(nz, 2, rows, part_cols)
                first_half, second_half = part[:, 0], part[:, 1]
                mine = jnp.where(x == 0, first_half, second_half)
                other = jnp.where(x == 0, second_half, first_half)
                own[c * sub + u] = mine
                rxs[t, c * sub + u] = other.astype(BF16)
                rx_copy(t, c * sub + u).start()

        over(0, chunks, body)

    def pair_sum(t, c):
        rx_copy(t, c).wait_recv()
        total = own[c] + rxr[t, c].astype(F32)
        own[c] = total
        rzs[t, c] = total.astype(BF16)
        for j in range(1, nz):
            rz_copy(t, c, j).start()

    def line_sum(t, c):
        total = own[c, z] + dyb[t, c, z, x].astype(F32)
        for j in range(1, nz):
            rz_copy(t, c, j).wait_recv()
            total = total + rzr[t, c, j].astype(F32)
        res[t, c] = total.astype(BF16)
        if t + 1 < slots:
            @pl.when(s > 0)
            def _():
                for j in range(nz):
                    sh_copy(t, c, j).start()

    def hand_over(t, c):
        for j in range(nz):
            sh_copy(t, c, j).wait_recv()
        af_copy(t, c).start()

    def example_mask(t):
        position = lax.broadcasted_iota(jnp.int32, (tokens, 1), 0)
        across = lax.broadcasted_iota(jnp.int32, (1, tokens), 1)
        down, along = [], []
        start = jnp.int32(0)
        for e in range(examples):
            stop = start + lengths_ref[0, e, t]
            if e == examples - 1:
                stop = jnp.int32(tokens)
            down.append((position >= start) & (position < stop))
            along.append((across >= start) & (across < stop))
            start = stop
        return down, along

    def sq_copy(t, j):
        return pltpu.make_async_remote_copy(sqs.at[t], sqr.at[t, j], sq_send.at[t, j], sq_recv.at[t, j], device_id={"section": s, "tensor": (p + j) % parts}, device_id_type=MESH)

    def grams(t):
        inputs = xg[t].reshape(tokens, width)
        gxs[...] = dot(inputs, inputs, NT)
        ghs[...] = dot(h[t], h[t], NT)

    def squares(t):
        grads = grads_of(t, 0, count)
        paired = gxs[...] * dot(dz[t], dz[t], NT) + ghs[...] * dot(grads, grads, NT)
        down, along = example_mask(t)
        row = lax.broadcasted_iota(jnp.int32, (8, 128), 0)
        out = jnp.zeros((8, 128), F32)
        for e in range(examples):
            kept = jnp.where(down[e], paired, 0.0)
            kept = jnp.where(along[e], kept, 0.0)
            value = jnp.sum(jnp.sum(kept, axis=0, keepdims=True), axis=1, keepdims=True)
            out = jnp.where(row == e, value, out)
        sqs[t] = out
        for j in range(1, parts):
            sq_copy(t, j).start()

    def factors(t):
        total = sqs[t]
        for j in range(1, parts):
            sq_copy(t, j).wait_recv()
            total = total + sqr[t, j]
        factor = 1.0 / (jnp.sqrt(total / (width * hidden_all)) + GAMMA)
        down, _ = example_mask(t)
        per_token = jnp.zeros((tokens, 1), F32)
        for e in range(examples):
            per_token = jnp.where(down[e], factor[e:e + 1, 0:1], per_token)
        return per_token

    def scale(t, k, per_token):
        at = slice(k * part_cols, (k + 1) * part_cols)
        scaled = xg[t, :, :, :, at].reshape(tokens, part_cols).astype(F32) * per_token
        xct[t, at] = scaled.T.astype(BF16)
        dyc[t, :, at] = (dyb[t, k].reshape(tokens, part_cols).astype(F32) * per_token).astype(BF16)

    def grad_in_block(i):
        at = pl.ds(i * span, span)
        lhs = jnp.concatenate([xct[t] for t in range(slots)], axis=1)
        rhs = jnp.concatenate([dz[t, :, at] for t in range(slots)], axis=0)
        win[:, at] = jnp.dot(lhs, rhs, preferred_element_type=F32).astype(BF16)

    def grad_out_block(i):
        at = pl.ds(i * span, span)
        lhs = jnp.concatenate([h[t, :, at] for t in range(slots)], axis=0)
        wout[at, :] = dot(lhs, dyc[...].reshape(slots * tokens, width), TN).astype(BF16)

    end = slots - 1
    ag_open(0)
    ag_open(slots)
    ag_forward(0)
    ag_forward(slots)
    if end > 0:
        ag_open(1)

        @pl.when(is_last)
        def _():
            ag_open(slots + 1)

    for k in range(pieces):
        pltpu.make_async_copy(win_hbm.at[0, :, pl.ds(k * span_in, span_in)], win.at[:, pl.ds(k * span_in, span_in)], w_sem.at[0, k]).wait()
    ag_finish(0)
    over(0, 2, lambda i: z_tile(0, i, local // 2))
    grams(0)
    for k in range(pieces):
        pltpu.make_async_copy(wout_hbm.at[0, pl.ds(k * span_out, span_out)], wout.at[pl.ds(k * span_out, span_out)], w_sem.at[1, k]).wait()
    ag_finish(slots)
    over(0, 2, lambda i: back_tile(0, i, local // 2))

    for t in range(end):
        partial_dx(t)
        if t > 0:
            grams(t)
        squares(t)
        ag_forward(t + 1)
        over(0, count, lambda k: pair_sum(t, k))

        @pl.when(is_last)
        def _():
            ag_forward(slots + t + 1)

        per_token = None
        for k in range(count):
            line_sum(t, k)
            if k == 1:
                per_token = factors(t)
            if k > 1:
                scale(t, k - 2, per_token)
        for k in range(count - 2, count):
            scale(t, k, per_token)
        ag_finish(t + 1)

        def tile_and_hand(c):
            @pl.when(s < sections - 1)
            def _():
                for u in range(sub):
                    hand_over(t, c * sub + u)

            z_tile(t + 1, c, span)

        over(0, chunks, tile_and_hand)
        if t + 2 < slots:
            ag_open(t + 2)

            @pl.when(is_last)
            def _():
                ag_open(slots + t + 2)

        if t + 1 == end:
            grams(end)

        @pl.when(is_last)
        def _():
            ag_finish(slots + t + 1)

        for c in range(chunks):
            @pl.when(s < sections - 1)
            def _():
                for u in range(sub):
                    af_copy(t, c * sub + u).wait_recv()

            back_chunk(t + 1, c, 0 if c == 0 else (2 if c == chunks - 1 else 1))

    squares(end)
    partial_dx(end)
    per_token = factors(end)
    for k in range(count):
        scale(end, k, per_token)
    for c in range(chunks):
        for k in range(count):
            if min(chunks - 1, (k + 2) // 3) == c:
                pair_sum(end, k)
        grad_in_block(c)
    for i in range(ready):
        grad_out_block(i)
    over(0, count, lambda k: line_sum(end, k))

    for t in range(slots):
        for c in range(count):
            res_ref[0, t, :, c * part_cols:(c + 1) * part_cols] = res[t, c]

    for t in range(slots):
        ag_drain(t)
    ag_drain(slots)

    @pl.when(is_last)
    def _():
        for t in range(1, slots):
            ag_drain(slots + t)

    for t in range(slots):
        def drain(c):
            rx_copy(t, c).wait_send()
            for j in range(1, nz):
                rz_copy(t, c, j).wait_send()

        over(0, count, drain)
        for j in range(1, parts):
            sq_copy(t, j).wait_send()
        if t + 1 < slots:
            @pl.when(s > 0)
            def _():
                def drain_shift(c):
                    for j in range(nz):
                        sh_copy(t, c, j).wait_send()

                over(0, count, drain_shift)

            @pl.when(s < sections - 1)
            def _():
                over(0, count, lambda c: af_copy(t, c).wait_send())


def finish_kernel(cfg, gin_ref, gout_ref, h, dyc, res_ref, gin_hbm, gout_hbm, res_hbm, made, sem):
    blocks, ready = cfg
    slots, tokens, local = h.shape
    width = dyc.shape[2]
    span = local // blocks
    step = width // blocks
    copies = []
    for i in range(ready):
        at = pl.ds(i * span, span)
        copies.append(pltpu.make_async_copy(gout_ref.at[0, at], gout_hbm.at[0, at], sem.at[1, i]))
    for i in range(blocks):
        at = pl.ds(i * step, step)
        copies.append(pltpu.make_async_copy(gin_ref.at[0, at], gin_hbm.at[0, at], sem.at[0, i]))
    copies.append(pltpu.make_async_copy(res_ref, res_hbm, sem.at[2, 0]))
    for copy in copies:
        copy.start()
    for i in range(ready, blocks):
        at = pl.ds(i * span, span)
        lhs = jnp.concatenate([h[t, :, at] for t in range(slots)], axis=0)
        made[i - ready] = dot(lhs, dyc[...].reshape(slots * tokens, width), TN).astype(BF16)
        copy = pltpu.make_async_copy(made.at[i - ready], gout_hbm.at[0, at], sem.at[1, i])
        copy.start()
        copies.append(copy)
    for copy in copies:
        copy.wait()


def fast_device(sections, saved_inputs, slot_index, example_lengths, first_grads, loss_grads, w_in, w_out):
    parts = lax.axis_size("tensor")
    slots = loss_grads.shape[0] + 1
    rows, width = first_grads.shape[1:]
    local = w_in.shape[2]
    nz = parts // 2
    tokens = parts * rows
    examples = example_lengths.shape[2]
    chunks = max(1, width // 256)
    sub = 1
    ready = min(1, chunks)
    count = chunks * sub
    part_cols = width // count
    cfg = (sections, parts, nz, slots, rows, width, local, chunks, sub, ready, examples, local * parts)
    hbm = pl.BlockSpec(memory_space=pl.ANY)
    vmem = pl.BlockSpec(memory_space=pltpu.VMEM)
    dma = pltpu.SemaphoreType.DMA
    sds = jax.ShapeDtypeStruct
    flops = 2 * tokens * width * local * slots * 5
    grad_in, grad_out, hidden, scaled, results = pl.pallas_call(
        functools.partial(chain_kernel, cfg),
        out_shape=(
            pltpu.VMEM((1, width, local), BF16),
            pltpu.VMEM((1, local, width), BF16),
            pltpu.VMEM((slots, tokens, local), BF16),
            pltpu.VMEM((slots, tokens, width), BF16),
            pltpu.VMEM((1, slots, rows, width), BF16),
        ),
        in_specs=[pl.BlockSpec(memory_space=pltpu.HBM)] * 7,
        out_specs=[vmem] * 5,
        scratch_shapes=[
            pltpu.VMEM((slots, nz, 2, rows, width), BF16),
            pltpu.VMEM((slots, count, nz, 2, rows, part_cols), BF16),
            pltpu.VMEM((slots, tokens, local), BF16),
            pltpu.VMEM((tokens, local), F32),
            pltpu.VMEM((tokens, local), F32),
            pltpu.VMEM((tokens, tokens), F32),
            pltpu.VMEM((tokens, tokens), F32),
            pltpu.VMEM((count, nz, rows, part_cols), F32),
            pltpu.VMEM((slots, count, nz, rows, part_cols), BF16),
            pltpu.VMEM((slots, count, nz, rows, part_cols), BF16),
            pltpu.VMEM((slots, count, nz, rows, part_cols), BF16),
            pltpu.VMEM((slots, count, nz, rows, part_cols), BF16),
            pltpu.VMEM((slots, count, rows, part_cols), BF16),
            pltpu.VMEM((slots, 8, 128), F32),
            pltpu.VMEM((slots, parts, 8, 128), F32),
            pltpu.VMEM((slots, width, tokens), BF16),
            pltpu.SMEM(slot_index.shape, jnp.int32),
            pltpu.SMEM((1, examples, slots), jnp.int32),
            pltpu.VMEM(saved_inputs.shape[1:], BF16),
            dma((3 + slots * count,)),
            dma((2, 4)),
            dma((2 * slots, nz)), dma((2 * slots, nz)), dma((2 * slots, nz)), dma((2 * slots, nz)),
            dma((slots, count)), dma((slots, count)),
            dma((slots, count, nz)), dma((slots, count, nz)),
            dma((slots - 1, count, nz)), dma((slots - 1, count, nz)),
            dma((slots - 1, count)), dma((slots - 1, count)),
            dma((slots, parts)), dma((slots, parts)),
        ],
        compiler_params=pltpu.CompilerParams(collective_id=0, has_side_effects=True, vmem_limit_bytes=36 * 1024 * 1024),
        cost_estimate=pl.CostEstimate(flops=flops, bytes_accessed=4 * width * local, transcendentals=0),
        name="chain",
    )(slot_index, jnp.swapaxes(example_lengths, 1, 2), saved_inputs, first_grads, loss_grads, w_in, w_out)

    return pl.pallas_call(
        functools.partial(finish_kernel, (chunks, ready)),
        out_shape=(
            sds((1, width, local), BF16),
            sds((1, local, width), BF16),
            sds((1, slots, rows, width), BF16),
        ),
        in_specs=[vmem] * 5,
        out_specs=[hbm] * 3,
        scratch_shapes=[pltpu.VMEM((chunks - ready, local // chunks, width), BF16), dma((3, chunks))],
        compiler_params=pltpu.CompilerParams(vmem_limit_bytes=8 * 1024 * 1024),
        cost_estimate=pl.CostEstimate(flops=2 * slots * tokens * width * local, bytes_accessed=8 * width * local, transcendentals=0),
        name="finish",
    )(grad_in, grad_out, hidden, scaled, results)


def shifted(value, axis, steps):
    count = lax.axis_size(axis)
    first, last = (max(0, -steps), min(count, count - steps))
    return lax.ppermute(value, axis, [(source, source + steps) for source in range(first, last)])


def membership(lengths, tokens):
    ends = jnp.cumsum(lengths)
    position = jnp.arange(tokens, dtype=jnp.int32)
    example_id = jnp.sum((position[:, None] >= ends[None, :-1]).astype(jnp.int32), axis=1)
    labels = jnp.arange(lengths.shape[0], dtype=jnp.int32)
    return (example_id[:, None] == labels[None, :]).astype(F32)


def spread(value, axis):
    copies = jnp.broadcast_to(value[None], (lax.axis_size(axis),) + value.shape)
    return lax.all_to_all(copies, axis, 0, 0)


def gram(value):
    return lax.dot_general(value, value, (((1,), (1,)), ((), ())), preferred_element_type=F32)


def per_device(saved_inputs, slot_index, example_lengths, first_grads, loss_grads, w_in, w_out):
    section_count = lax.axis_size("section")
    parts = lax.axis_size("tensor")
    is_last = lax.axis_index("section") == section_count - 1
    first = w_in[0]
    second = w_out[0]
    slot_count = loss_grads.shape[0] + 1
    rows, width = first_grads.shape[1:]
    hidden_all = first.shape[1] * parts
    picked = [
        lax.dynamic_index_in_dim(saved_inputs[0], slot_index[0, slot], 0, keepdims=False)
        for slot in range(slot_count)
    ]
    tokens = parts * rows
    opening = spread(jnp.concatenate([picked[0], first_grads[0]]), "tensor")
    later = spread(jnp.concatenate(picked[1:]), "tensor")
    every_input = [opening[:, :rows].reshape(tokens, width)]
    for slot in range(slot_count - 1):
        every_input.append(later[:, slot * rows : (slot + 1) * rows].reshape(tokens, width))
    incoming = first_grads[0]
    results, dzs, hiddens, grad_list, members, squares = [], [], [], [], [], []
    for slot in range(slot_count):
        inputs = every_input[slot]
        if slot == 0:
            grads = opening[:, rows:].reshape(tokens, width)
        else:
            grads = spread(incoming, "tensor").reshape(tokens, width)
        z = jnp.dot(inputs, first, preferred_element_type=F32)
        relu = jnp.maximum(z, 0.0)
        hidden = (relu * relu).astype(BF16)
        back = jnp.einsum("td,fd->tf", grads, second, preferred_element_type=F32)
        dz = (2.0 * relu * back).astype(BF16)
        own_terms = jnp.einsum("tf,df->td", dz, first, preferred_element_type=F32).astype(BF16)
        pieces = lax.all_to_all(own_terms.reshape(parts, rows, width), "tensor", 0, 0)
        shares = jnp.sum(pieces.astype(F32), axis=0)
        passing = (incoming.astype(F32) + shares).astype(BF16)
        results.append(passing)
        if slot + 1 < slot_count:
            arrived = shifted(passing, "section", -1)
            incoming = jnp.where(is_last, loss_grads[slot], arrived)
        member = membership(example_lengths[0, slot], inputs.shape[0])
        paired = gram(inputs) * gram(dz) + gram(hidden) * gram(grads)
        per_row = jnp.stack([jnp.sum(paired * member[:, e][None, :], axis=1) for e in range(member.shape[1])], axis=1)
        squares.append(jnp.sum(member * per_row, axis=0))
        dzs.append(dz)
        hiddens.append(hidden)
        grad_list.append(grads)
        members.append(member)
    local = jnp.stack(squares)
    total = jnp.sum(spread(local, "tensor"), axis=0)
    factor = 1.0 / (jnp.sqrt(total / (width * hidden_all)) + GAMMA)
    token_factor = jnp.concatenate([jnp.sum(m * factor[i][None, :], axis=1) for i, m in enumerate(members)])[:, None]
    xc = (jnp.concatenate(every_input).astype(F32) * token_factor).astype(BF16)
    dyc = (jnp.concatenate(grad_list).astype(F32) * token_factor).astype(BF16)
    grad_in = jnp.einsum("td,tf->df", xc, jnp.concatenate(dzs), preferred_element_type=F32).astype(BF16)[None]
    grad_out = jnp.einsum("tf,td->fd", jnp.concatenate(hiddens), dyc, preferred_element_type=F32).astype(BF16)[None]
    input_grads = jnp.stack(results)[None]
    return (grad_in, grad_out, input_grads)


def solution(mesh):
    sections = mesh.shape["section"]
    parts = mesh.shape["tensor"]

    def body(saved_inputs, slot_index, example_lengths, first_grads, loss_grads, w_in, w_out):
        rows, width = first_grads.shape[1:]
        fits = sections > 2 and parts % 2 == 0 and rows % 16 == 0 and width % 256 == 0 and w_in.shape[2] % 512 == 0 and loss_grads.shape[0] > 0
        run = functools.partial(fast_device, sections) if fits else per_device
        return run(saved_inputs, slot_index, example_lengths, first_grads, loss_grads, w_in, w_out)

    return jax.shard_map(
        body,
        mesh=mesh,
        in_specs=(
            P("section", None, "tensor", None),
            P("section", None),
            P("section", None, None),
            P("section", "tensor", None),
            P(None, "tensor", None),
            P("section", None, "tensor"),
            P("section", "tensor", None),
        ),
        out_specs=(
            P("section", None, "tensor"),
            P("section", "tensor", None),
            P("section", None, "tensor", None),
        ),
        check_vma=False,
    )
```

```python
import functools

import jax
import jax.numpy as jnp
from jax import lax
from jax.experimental import pallas as pl
from jax.experimental.pallas import tpu as pltpu
from jax.sharding import PartitionSpec as P

GAMMA = 0.01
F32 = jnp.float32
BF16 = jnp.bfloat16
MESH = pl.DeviceIdType.MESH
NT = (((1,), (1,)), ((), ()))
TN = (((0,), (0,)), ((), ()))


def dot(a, b, dims):
    return lax.dot_general(a, b, dims, preferred_element_type=F32)


def chain_kernel(
    cfg,
    index_hbm, lengths_hbm, saved_hbm, first_hbm, loss_hbm, win_hbm, wout_hbm,
    gin_ref, gout_ref, h, dyc, res_ref,
    xg, dyb, dz, rbuf, acc, gxs, ghs, own, rxs, rxr, rzs, rzr, res, sqs, sqr, xct,
    index_ref, lengths_ref, saved_ref, in_sem,
    w_sem, ag_send, ag_recv, fw_send, fw_recv, rx_send, rx_recv, rz_send, rz_recv,
    sh_send, sh_recv, af_send, af_recv, sq_send, sq_recv,
):
    sections, parts, nz, slots, rows, width, local, chunks, sub, ready, examples, hidden_all = cfg
    cols = width // chunks
    count = chunks * sub
    part_cols = cols // sub
    tokens = parts * rows
    win, wout = gin_ref.at[0], gout_ref.at[0]
    span = local // chunks
    s = lax.axis_index("section")
    p = lax.axis_index("tensor")
    z = p // 2
    x = p % 2
    is_last = s == sections - 1
    partner = {"section": s, "tensor": z * 2 + (1 - x)}

    def zpeer(j):
        return {"section": s, "tensor": ((z + j) % nz) * 2 + x}

    def behind(j):
        return {"section": s - 1, "tensor": ((z + j) % nz) * 2 + x}

    index_in = pltpu.make_async_copy(index_hbm, index_ref, in_sem.at[0])
    lengths_in = pltpu.make_async_copy(lengths_hbm, lengths_ref, in_sem.at[1])
    saved_in = pltpu.make_async_copy(saved_hbm.at[0], saved_ref, in_sem.at[2])
    index_in.start()
    saved_in.start()
    lengths_in.start()

    def grads_in(t, c):
        source = first_hbm.at[0] if t == 0 else loss_hbm.at[t - 1]
        return pltpu.make_async_copy(source.at[:, c * part_cols:(c + 1) * part_cols], dyb.at[t, c, z, x], in_sem.at[3 + t * count + c])

    for c in range(count):
        grads_in(0, c).start()

    @pl.when(is_last)
    def _():
        for t in range(1, slots):
            for c in range(count):
                grads_in(t, c).start()

    pieces = 4
    span_in, span_out = local // pieces, local // pieces
    for k in range(pieces):
        pltpu.make_async_copy(win_hbm.at[0, :, pl.ds(k * span_in, span_in)], win.at[:, pl.ds(k * span_in, span_in)], w_sem.at[0, k]).start()
    for k in range(pieces):
        pltpu.make_async_copy(wout_hbm.at[0, pl.ds(k * span_out, span_out)], wout.at[pl.ds(k * span_out, span_out)], w_sem.at[1, k]).start()

    barrier = pltpu.get_barrier_semaphore()
    for j in range(1, parts):
        pl.semaphore_signal(barrier, inc=1, device_id={"section": s, "tensor": (p + j) % parts}, device_id_type=MESH)

    for side in (1, sections - 1):
        for j in range(nz):
            pl.semaphore_signal(barrier, inc=1, device_id={"section": (s + side) % sections, "tensor": ((z + j) % nz) * 2 + x}, device_id_type=MESH)
    index_in.wait()
    saved_in.wait()
    for t in range(slots):
        xg[t, z, x] = saved_ref[index_ref[0, t]]
    for c in range(count):
        grads_in(0, c).wait()
    lengths_in.wait()

    @pl.when(is_last)
    def _():
        for t in range(1, slots):
            for c in range(count):
                grads_in(t, c).wait()

    pl.semaphore_wait(barrier, parts - 1 + 2 * nz)

    def block(k, source):
        if k < slots:
            return xg.at[k, source, x]
        return dyb.at[k - slots, :, source, x]

    def ag_copy(k, j, to_partner):
        if to_partner:
            ref = block(k, (z + nz - j) % nz)
            return pltpu.make_async_remote_copy(ref, ref, fw_send.at[k, j], fw_recv.at[k, j], device_id=partner, device_id_type=MESH)
        ref = block(k, z)
        return pltpu.make_async_remote_copy(ref, ref, ag_send.at[k, j], ag_recv.at[k, j], device_id=zpeer(j), device_id_type=MESH)

    def ag_open(k):
        for j in range(1, nz):
            ag_copy(k, j, False).start()

    def ag_forward(k):
        ag_copy(k, 0, True).start()
        for j in range(1, nz):
            ag_copy(k, j, False).wait_recv()
            ag_copy(k, j, True).start()

    def ag_finish(k):
        for j in range(nz):
            ag_copy(k, j, True).wait_recv()

    def ag_drain(k):
        for j in range(nz):
            if j:
                ag_copy(k, j, False).wait_send()
            ag_copy(k, j, True).wait_send()

    def grads_of(t, lo, hi):
        return jnp.concatenate([dyb[t, c].reshape(tokens, part_cols) for c in range(lo, hi)], axis=1)

    def z_tile(t, i, size):
        at = pl.ds(pl.multiple_of(i * size, size), size)
        zz = jnp.dot(xg[t].reshape(tokens, width), win[:, at], preferred_element_type=F32)
        r = jnp.maximum(zz, 0.0)
        rbuf[:, at] = r
        h[t, :, at] = (r * r).astype(BF16)

    def back_tile(t, i, size):
        at = pl.ds(pl.multiple_of(i * size, size), size)
        dh = dot(grads_of(t, 0, count), wout[at, :], NT)
        dz[t, :, at] = (2.0 * rbuf[:, at] * dh).astype(BF16)

    def back_chunk(t, c, mode):
        size = min(2048, local)

        def body(i, carry):
            at = pl.ds(pl.multiple_of(i * size, size), size)
            dh = dot(grads_of(t, c * sub, (c + 1) * sub), wout[at, c * cols:(c + 1) * cols], NT)
            if mode > 0:
                dh = dh + acc[:, at]
            if mode < 2:
                acc[:, at] = dh
            else:
                dz[t, :, at] = (2.0 * rbuf[:, at] * dh).astype(BF16)
            return carry

        lax.fori_loop(0, local // size, body, 0)

    def rx_copy(t, c):
        return pltpu.make_async_remote_copy(rxs.at[t, c], rxr.at[t, c], rx_send.at[t, c], rx_recv.at[t, c], device_id=partner, device_id_type=MESH)

    def rz_copy(t, c, j):
        return pltpu.make_async_remote_copy(rzs.at[t, c, (z + j) % nz], rzr.at[t, c, j], rz_send.at[t, c, j], rz_recv.at[t, c, j], device_id=zpeer(j), device_id_type=MESH)

    def sh_copy(t, c, j):
        return pltpu.make_async_remote_copy(res.at[t, c], dyb.at[t + 1, c, z, x], sh_send.at[t, c, j], sh_recv.at[t, c, j], device_id=behind(j), device_id_type=MESH)

    def af_copy(t, c):
        ref = dyb.at[t + 1, c, :, x]
        return pltpu.make_async_remote_copy(ref, ref, af_send.at[t, c], af_recv.at[t, c], device_id=partner, device_id_type=MESH)

    def over(lo, hi, body):
        def step(c, carry):
            body(c)
            return carry

        lax.fori_loop(lo, hi, step, 0)

    def partial_dx(t):
        def body(c):
            wide = win[pl.ds(pl.multiple_of(c * cols, cols), cols), :]
            whole = dot(dz[t], wide, NT)
            for u in range(sub):
                part = whole[:, u * part_cols:(u + 1) * part_cols].reshape(nz, 2, rows, part_cols)
                first_half, second_half = part[:, 0], part[:, 1]
                mine = jnp.where(x == 0, first_half, second_half)
                other = jnp.where(x == 0, second_half, first_half)
                own[c * sub + u] = mine
                rxs[t, c * sub + u] = other.astype(BF16)
                rx_copy(t, c * sub + u).start()

        over(0, chunks, body)

    def pair_sum(t, c):
        rx_copy(t, c).wait_recv()
        total = own[c] + rxr[t, c].astype(F32)
        own[c] = total
        rzs[t, c] = total.astype(BF16)
        for j in range(1, nz):
            rz_copy(t, c, j).start()

    def line_sum(t, c):
        total = own[c, z] + dyb[t, c, z, x].astype(F32)
        for j in range(1, nz):
            rz_copy(t, c, j).wait_recv()
            total = total + rzr[t, c, j].astype(F32)
        res[t, c] = total.astype(BF16)
        if t + 1 < slots:
            @pl.when(s > 0)
            def _():
                for j in range(nz):
                    sh_copy(t, c, j).start()

    def hand_over(t, c):
        for j in range(nz):
            sh_copy(t, c, j).wait_recv()
        af_copy(t, c).start()

    def example_mask(t):
        position = lax.broadcasted_iota(jnp.int32, (tokens, 1), 0)
        across = lax.broadcasted_iota(jnp.int32, (1, tokens), 1)
        down, along = [], []
        start = jnp.int32(0)
        for e in range(examples):
            stop = start + lengths_ref[0, e, t]
            if e == examples - 1:
                stop = jnp.int32(tokens)
            down.append((position >= start) & (position < stop))
            along.append((across >= start) & (across < stop))
            start = stop
        return down, along

    def sq_copy(t, j):
        return pltpu.make_async_remote_copy(sqs.at[t], sqr.at[t, j], sq_send.at[t, j], sq_recv.at[t, j], device_id={"section": s, "tensor": (p + j) % parts}, device_id_type=MESH)

    def grams(t):
        inputs = xg[t].reshape(tokens, width)
        gxs[...] = dot(inputs, inputs, NT)
        ghs[...] = dot(h[t], h[t], NT)

    def squares(t):
        grads = grads_of(t, 0, count)
        paired = gxs[...] * dot(dz[t], dz[t], NT) + ghs[...] * dot(grads, grads, NT)
        down, along = example_mask(t)
        row = lax.broadcasted_iota(jnp.int32, (8, 128), 0)
        out = jnp.zeros((8, 128), F32)
        for e in range(examples):
            kept = jnp.where(down[e], paired, 0.0)
            kept = jnp.where(along[e], kept, 0.0)
            value = jnp.sum(jnp.sum(kept, axis=0, keepdims=True), axis=1, keepdims=True)
            out = jnp.where(row == e, value, out)
        sqs[t] = out
        for j in range(1, parts):
            sq_copy(t, j).start()

    def factors(t):
        total = sqs[t]
        for j in range(1, parts):
            sq_copy(t, j).wait_recv()
            total = total + sqr[t, j]
        factor = 1.0 / (jnp.sqrt(total / (width * hidden_all)) + GAMMA)
        down, _ = example_mask(t)
        per_token = jnp.zeros((tokens, 1), F32)
        for e in range(examples):
            per_token = jnp.where(down[e], factor[e:e + 1, 0:1], per_token)
        return per_token

    def scale(t, k, per_token):
        at = slice(k * part_cols, (k + 1) * part_cols)
        scaled = xg[t, :, :, :, at].reshape(tokens, part_cols).astype(F32) * per_token
        xct[t, at] = scaled.T.astype(BF16)
        dyc[t, :, at] = (dyb[t, k].reshape(tokens, part_cols).astype(F32) * per_token).astype(BF16)

    def grad_in_block(i):
        at = pl.ds(i * span, span)
        lhs = jnp.concatenate([xct[t] for t in range(slots)], axis=1)
        rhs = jnp.concatenate([dz[t, :, at] for t in range(slots)], axis=0)
        win[:, at] = jnp.dot(lhs, rhs, preferred_element_type=F32).astype(BF16)

    def grad_out_block(i):
        at = pl.ds(i * span, span)
        lhs = jnp.concatenate([h[t, :, at] for t in range(slots)], axis=0)
        wout[at, :] = dot(lhs, dyc[...].reshape(slots * tokens, width), TN).astype(BF16)

    end = slots - 1
    ag_open(0)
    ag_open(slots)
    ag_forward(0)
    ag_forward(slots)
    if end > 0:
        ag_open(1)

        @pl.when(is_last)
        def _():
            ag_open(slots + 1)

    for k in range(pieces):
        pltpu.make_async_copy(win_hbm.at[0, :, pl.ds(k * span_in, span_in)], win.at[:, pl.ds(k * span_in, span_in)], w_sem.at[0, k]).wait()
    ag_finish(0)
    over(0, 2, lambda i: z_tile(0, i, local // 2))
    grams(0)
    for k in range(pieces):
        pltpu.make_async_copy(wout_hbm.at[0, pl.ds(k * span_out, span_out)], wout.at[pl.ds(k * span_out, span_out)], w_sem.at[1, k]).wait()
    ag_finish(slots)
    over(0, 2, lambda i: back_tile(0, i, local // 2))

    for t in range(end):
        partial_dx(t)
        if t == 0:
            ag_forward(t + 1)
        else:
            grams(t)
        squares(t)
        if t > 0:
            ag_forward(t + 1)
        over(0, count, lambda k: pair_sum(t, k))

        @pl.when(is_last)
        def _():
            ag_forward(slots + t + 1)

        per_token = None
        for k in range(count):
            line_sum(t, k)
            if k == 1:
                per_token = factors(t)
            if k > 1:
                scale(t, k - 2, per_token)
        for k in range(count - 2, count):
            scale(t, k, per_token)
        ag_finish(t + 1)

        def tile_and_hand(c):
            @pl.when(s < sections - 1)
            def _():
                for u in range(sub):
                    hand_over(t, c * sub + u)

            z_tile(t + 1, c, span)

        over(0, chunks, tile_and_hand)
        if t + 2 < slots:
            ag_open(t + 2)

            @pl.when(is_last)
            def _():
                ag_open(slots + t + 2)

        if t + 1 == end:
            grams(end)

        @pl.when(is_last)
        def _():
            ag_finish(slots + t + 1)

        for c in range(chunks):
            @pl.when(s < sections - 1)
            def _():
                for u in range(sub):
                    af_copy(t, c * sub + u).wait_recv()

            back_chunk(t + 1, c, 0 if c == 0 else (2 if c == chunks - 1 else 1))

    squares(end)
    partial_dx(end)
    per_token = factors(end)
    for k in range(count):
        scale(end, k, per_token)
    for c in range(chunks):
        for k in range(count):
            if min(chunks - 1, (k + 2) // 3) == c:
                pair_sum(end, k)
        grad_in_block(c)
    for i in range(ready):
        grad_out_block(i)
    over(0, count, lambda k: line_sum(end, k))

    for t in range(slots):
        for c in range(count):
            res_ref[0, t, :, c * part_cols:(c + 1) * part_cols] = res[t, c]

    for t in range(slots):
        ag_drain(t)
    ag_drain(slots)

    @pl.when(is_last)
    def _():
        for t in range(1, slots):
            ag_drain(slots + t)

    for t in range(slots):
        def drain(c):
            rx_copy(t, c).wait_send()
            for j in range(1, nz):
                rz_copy(t, c, j).wait_send()

        over(0, count, drain)
        for j in range(1, parts):
            sq_copy(t, j).wait_send()
        if t + 1 < slots:
            @pl.when(s > 0)
            def _():
                def drain_shift(c):
                    for j in range(nz):
                        sh_copy(t, c, j).wait_send()

                over(0, count, drain_shift)

            @pl.when(s < sections - 1)
            def _():
                over(0, count, lambda c: af_copy(t, c).wait_send())


def finish_kernel(cfg, gin_ref, gout_ref, h, dyc, res_ref, gin_hbm, gout_hbm, res_hbm, made, sem):
    blocks, ready = cfg
    slots, tokens, local = h.shape
    width = dyc.shape[2]
    span = local // blocks
    step = width // blocks
    copies = []
    for i in range(ready):
        at = pl.ds(i * span, span)
        copies.append(pltpu.make_async_copy(gout_ref.at[0, at], gout_hbm.at[0, at], sem.at[1, i]))
    for i in range(blocks):
        at = pl.ds(i * step, step)
        copies.append(pltpu.make_async_copy(gin_ref.at[0, at], gin_hbm.at[0, at], sem.at[0, i]))
    copies.append(pltpu.make_async_copy(res_ref, res_hbm, sem.at[2, 0]))
    for copy in copies:
        copy.start()
    half = span // 2
    pieces = [(i * span, span) for i in range(ready, blocks - 1)] + [((blocks - 1) * span, half), (blocks * span - half, half)]
    for i, (start, size) in enumerate(pieces):
        at = pl.ds(start, size)
        to = pl.ds(start - ready * span, size)
        lhs = jnp.concatenate([h[t, :, at] for t in range(slots)], axis=0)
        made[to] = dot(lhs, dyc[...].reshape(slots * tokens, width), TN).astype(BF16)
        copy = pltpu.make_async_copy(made.at[to], gout_hbm.at[0, at], sem.at[1, ready + i])
        copy.start()
        copies.append(copy)
    for copy in copies:
        copy.wait()


def fast_device(sections, saved_inputs, slot_index, example_lengths, first_grads, loss_grads, w_in, w_out):
    parts = lax.axis_size("tensor")
    slots = loss_grads.shape[0] + 1
    rows, width = first_grads.shape[1:]
    local = w_in.shape[2]
    nz = parts // 2
    tokens = parts * rows
    examples = example_lengths.shape[2]
    chunks = max(1, width // 256)
    sub = 1
    ready = min(1, chunks)
    count = chunks * sub
    part_cols = width // count
    cfg = (sections, parts, nz, slots, rows, width, local, chunks, sub, ready, examples, local * parts)
    hbm = pl.BlockSpec(memory_space=pl.ANY)
    vmem = pl.BlockSpec(memory_space=pltpu.VMEM)
    dma = pltpu.SemaphoreType.DMA
    sds = jax.ShapeDtypeStruct
    flops = 2 * tokens * width * local * slots * 5
    grad_in, grad_out, hidden, scaled, results = pl.pallas_call(
        functools.partial(chain_kernel, cfg),
        out_shape=(
            pltpu.VMEM((1, width, local), BF16),
            pltpu.VMEM((1, local, width), BF16),
            pltpu.VMEM((slots, tokens, local), BF16),
            pltpu.VMEM((slots, tokens, width), BF16),
            pltpu.VMEM((1, slots, rows, width), BF16),
        ),
        in_specs=[pl.BlockSpec(memory_space=pltpu.HBM)] * 7,
        out_specs=[vmem] * 5,
        scratch_shapes=[
            pltpu.VMEM((slots, nz, 2, rows, width), BF16),
            pltpu.VMEM((slots, count, nz, 2, rows, part_cols), BF16),
            pltpu.VMEM((slots, tokens, local), BF16),
            pltpu.VMEM((tokens, local), F32),
            pltpu.VMEM((tokens, local), F32),
            pltpu.VMEM((tokens, tokens), F32),
            pltpu.VMEM((tokens, tokens), F32),
            pltpu.VMEM((count, nz, rows, part_cols), F32),
            pltpu.VMEM((slots, count, nz, rows, part_cols), BF16),
            pltpu.VMEM((slots, count, nz, rows, part_cols), BF16),
            pltpu.VMEM((slots, count, nz, rows, part_cols), BF16),
            pltpu.VMEM((slots, count, nz, rows, part_cols), BF16),
            pltpu.VMEM((slots, count, rows, part_cols), BF16),
            pltpu.VMEM((slots, 8, 128), F32),
            pltpu.VMEM((slots, parts, 8, 128), F32),
            pltpu.VMEM((slots, width, tokens), BF16),
            pltpu.SMEM(slot_index.shape, jnp.int32),
            pltpu.SMEM((1, examples, slots), jnp.int32),
            pltpu.VMEM(saved_inputs.shape[1:], BF16),
            dma((3 + slots * count,)),
            dma((2, 4)),
            dma((2 * slots, nz)), dma((2 * slots, nz)), dma((2 * slots, nz)), dma((2 * slots, nz)),
            dma((slots, count)), dma((slots, count)),
            dma((slots, count, nz)), dma((slots, count, nz)),
            dma((slots - 1, count, nz)), dma((slots - 1, count, nz)),
            dma((slots - 1, count)), dma((slots - 1, count)),
            dma((slots, parts)), dma((slots, parts)),
        ],
        compiler_params=pltpu.CompilerParams(collective_id=0, has_side_effects=True, vmem_limit_bytes=36 * 1024 * 1024),
        cost_estimate=pl.CostEstimate(flops=flops, bytes_accessed=4 * width * local, transcendentals=0),
        name="chain",
    )(slot_index, jnp.swapaxes(example_lengths, 1, 2), saved_inputs, first_grads, loss_grads, w_in, w_out)

    return pl.pallas_call(
        functools.partial(finish_kernel, (chunks, ready)),
        out_shape=(
            sds((1, width, local), BF16),
            sds((1, local, width), BF16),
            sds((1, slots, rows, width), BF16),
        ),
        in_specs=[vmem] * 5,
        out_specs=[hbm] * 3,
        scratch_shapes=[pltpu.VMEM(((chunks - ready) * (local // chunks), width), BF16), dma((3, chunks + 1))],
        compiler_params=pltpu.CompilerParams(vmem_limit_bytes=8 * 1024 * 1024),
        cost_estimate=pl.CostEstimate(flops=2 * slots * tokens * width * local, bytes_accessed=8 * width * local, transcendentals=0),
        name="finish",
    )(grad_in, grad_out, hidden, scaled, results)


def shifted(value, axis, steps):
    count = lax.axis_size(axis)
    first, last = (max(0, -steps), min(count, count - steps))
    return lax.ppermute(value, axis, [(source, source + steps) for source in range(first, last)])


def membership(lengths, tokens):
    ends = jnp.cumsum(lengths)
    position = jnp.arange(tokens, dtype=jnp.int32)
    example_id = jnp.sum((position[:, None] >= ends[None, :-1]).astype(jnp.int32), axis=1)
    labels = jnp.arange(lengths.shape[0], dtype=jnp.int32)
    return (example_id[:, None] == labels[None, :]).astype(F32)


def spread(value, axis):
    copies = jnp.broadcast_to(value[None], (lax.axis_size(axis),) + value.shape)
    return lax.all_to_all(copies, axis, 0, 0)


def gram(value):
    return lax.dot_general(value, value, (((1,), (1,)), ((), ())), preferred_element_type=F32)


def per_device(saved_inputs, slot_index, example_lengths, first_grads, loss_grads, w_in, w_out):
    section_count = lax.axis_size("section")
    parts = lax.axis_size("tensor")
    is_last = lax.axis_index("section") == section_count - 1
    first = w_in[0]
    second = w_out[0]
    slot_count = loss_grads.shape[0] + 1
    rows, width = first_grads.shape[1:]
    hidden_all = first.shape[1] * parts
    picked = [
        lax.dynamic_index_in_dim(saved_inputs[0], slot_index[0, slot], 0, keepdims=False)
        for slot in range(slot_count)
    ]
    tokens = parts * rows
    opening = spread(jnp.concatenate([picked[0], first_grads[0]]), "tensor")
    later = spread(jnp.concatenate(picked[1:]), "tensor")
    every_input = [opening[:, :rows].reshape(tokens, width)]
    for slot in range(slot_count - 1):
        every_input.append(later[:, slot * rows : (slot + 1) * rows].reshape(tokens, width))
    incoming = first_grads[0]
    results, dzs, hiddens, grad_list, members, squares = [], [], [], [], [], []
    for slot in range(slot_count):
        inputs = every_input[slot]
        if slot == 0:
            grads = opening[:, rows:].reshape(tokens, width)
        else:
            grads = spread(incoming, "tensor").reshape(tokens, width)
        z = jnp.dot(inputs, first, preferred_element_type=F32)
        relu = jnp.maximum(z, 0.0)
        hidden = (relu * relu).astype(BF16)
        back = jnp.einsum("td,fd->tf", grads, second, preferred_element_type=F32)
        dz = (2.0 * relu * back).astype(BF16)
        own_terms = jnp.einsum("tf,df->td", dz, first, preferred_element_type=F32).astype(BF16)
        pieces = lax.all_to_all(own_terms.reshape(parts, rows, width), "tensor", 0, 0)
        shares = jnp.sum(pieces.astype(F32), axis=0)
        passing = (incoming.astype(F32) + shares).astype(BF16)
        results.append(passing)
        if slot + 1 < slot_count:
            arrived = shifted(passing, "section", -1)
            incoming = jnp.where(is_last, loss_grads[slot], arrived)
        member = membership(example_lengths[0, slot], inputs.shape[0])
        paired = gram(inputs) * gram(dz) + gram(hidden) * gram(grads)
        per_row = jnp.stack([jnp.sum(paired * member[:, e][None, :], axis=1) for e in range(member.shape[1])], axis=1)
        squares.append(jnp.sum(member * per_row, axis=0))
        dzs.append(dz)
        hiddens.append(hidden)
        grad_list.append(grads)
        members.append(member)
    local = jnp.stack(squares)
    total = jnp.sum(spread(local, "tensor"), axis=0)
    factor = 1.0 / (jnp.sqrt(total / (width * hidden_all)) + GAMMA)
    token_factor = jnp.concatenate([jnp.sum(m * factor[i][None, :], axis=1) for i, m in enumerate(members)])[:, None]
    xc = (jnp.concatenate(every_input).astype(F32) * token_factor).astype(BF16)
    dyc = (jnp.concatenate(grad_list).astype(F32) * token_factor).astype(BF16)
    grad_in = jnp.einsum("td,tf->df", xc, jnp.concatenate(dzs), preferred_element_type=F32).astype(BF16)[None]
    grad_out = jnp.einsum("tf,td->fd", jnp.concatenate(hiddens), dyc, preferred_element_type=F32).astype(BF16)[None]
    input_grads = jnp.stack(results)[None]
    return (grad_in, grad_out, input_grads)


def solution(mesh):
    sections = mesh.shape["section"]
    parts = mesh.shape["tensor"]

    def body(saved_inputs, slot_index, example_lengths, first_grads, loss_grads, w_in, w_out):
        rows, width = first_grads.shape[1:]
        fits = sections > 2 and parts % 2 == 0 and rows % 16 == 0 and width % 256 == 0 and w_in.shape[2] % 512 == 0 and loss_grads.shape[0] > 0
        run = functools.partial(fast_device, sections) if fits else per_device
        return run(saved_inputs, slot_index, example_lengths, first_grads, loss_grads, w_in, w_out)

    return jax.shard_map(
        body,
        mesh=mesh,
        in_specs=(
            P("section", None, "tensor", None),
            P("section", None),
            P("section", None, None),
            P("section", "tensor", None),
            P(None, "tensor", None),
            P("section", None, "tensor"),
            P("section", "tensor", None),
        ),
        out_specs=(
            P("section", None, "tensor"),
            P("section", "tensor", None),
            P("section", None, "tensor", None),
        ),
        check_vma=False,
    )
```
